512 devices in a mesh: seq: 128 (over z, y, core), mp: 4 (over x).
Axes of the slice: x: 4, y: 8, z: 8, core: 2. Of those that a mesh axis runs over, the one named last changes fastest.
Arguments:
- y_first: bfloat16 [32768, 896], P('seq', 'mp'), may hold values from -6 to 6
- y_second: bfloat16 [32768, 896], P('seq', 'mp'), may hold values from -10 to 10
- grad_first: bfloat16 [32768, 896], P('seq', 'mp'), may hold values from -6 to 6
- grad_second: bfloat16 [32768, 896], P('seq', 'mp'), may hold values from -6 to 6
- doc_blocks: int32 [192], replicated, may hold values from 1 to 2, as said below
- last_fill: int32 [192], replicated, may hold values from 1 to 128
- plan: int32 [256], replicated, may hold values from 0 to 255, as said below
- q_weight: bfloat16 [896, 512], P(None, 'mp'), may hold values from -1 to 1
- kv_weight: bfloat16 [2, 896, 128], P(None, 'mp'), may hold values from -1 to 1
- out_weight: bfloat16 [512, 896], P('mp'), may hold values from -0.25 to 0.25
- gate_up: bfloat16 [2, 896, 2560], P(None, None, 'mp'), may hold values from -0.1875 to 0.1875
- down_weight: bfloat16 [2560, 896], P('mp'), may hold values from -0.125 to 0.125
Outputs:
- first_input: bfloat16 [32768, 896], P('seq', 'mp')
- second_input: bfloat16 [32768, 896], P('seq', 'mp')
- first_grad: bfloat16 [32768, 896], P('seq', 'mp')
- second_grad: bfloat16 [32768, 896], P('seq', 'mp')
- q_weight_grad: float32 [896, 512], P('seq', 'mp')
- kv_weight_grad: float32 [2, 896, 128], P(None, 'seq')
- out_weight_grad: float32 [512, 896], P('mp', 'seq')
The draws below stay inside these ranges and needn't reach their ends.
Inputs may be any that keep to these rules, and one draw needn't show every extreme that they name: `doc_blocks`: each document holds 1 or 2 blocks; together they fill all 256 blocks; exactly 64 documents hold 2. A permutation: block b goes to slot plan[b]; slots k * 2 to (k + 1) * 2 - 1 belong to index k of seq; the blocks of one document go to consecutive slots of one index, in order, the first at an even slot.
All inputs are finite; a program needn't handle non-finite values.
Results may differ from the reference program's by a relative error of at most 0.024.
Values may be sent and summed in bfloat16 or wider, within the bound.
No kernel may reach another device: no remote copies, remote signals or barrier semaphores. Data moves between devices by JAX's collectives and lax.ppermute only.
A program may use at most 64 MiB of HBM per device.

```python
import math
import jax
import jax.numpy as jnp
from jax import lax

D = 896
HD = 64
QH = 8
KVH = 2
FFW = 2560
BLOCK = 128
SLOTS = 2
TOKENS = 32768
BLOCKS = 256
DOCS = 192
N_SEQ = 128


def layout_draw(key):
    layout_key = jax.random.fold_in(key, 11)
    rank = jax.random.permutation(jax.random.fold_in(layout_key, 1), DOCS).astype(jnp.int32)
    paired = BLOCKS - DOCS
    counts = jnp.where(rank < paired, 2, 1).astype(jnp.int32)
    starts = (jnp.cumsum(counts) - counts).astype(jnp.int32)
    index = jnp.arange(BLOCKS, dtype=jnp.int32)
    owner_doc = (jnp.sum((starts[None, :] <= index[:, None]).astype(jnp.int32), axis=1) - 1).astype(jnp.int32)
    onehot = (owner_doc[:, None] == jnp.arange(DOCS, dtype=jnp.int32)[None, :]).astype(jnp.int32)
    offset = (index - jnp.sum(onehot * starts[None, :], axis=1)).astype(jnp.int32)
    block_rank = jnp.sum(onehot * rank[None, :], axis=1).astype(jnp.int32)
    virtual = jnp.where(block_rank < paired, 2 * block_rank + offset, block_rank + paired).astype(jnp.int32)
    owners = jax.random.permutation(jax.random.fold_in(layout_key, 2), N_SEQ).astype(jnp.int32)
    placed = owners[virtual // SLOTS] * SLOTS + virtual % SLOTS
    return (counts, placed.astype(jnp.int32))


def plant_parts(key):
    plant_key = jax.random.fold_in(key, 31)
    flips = jax.random.bernoulli(jax.random.fold_in(plant_key, 1), 0.5, (D,))
    direction = jnp.where(flips, 1.0, -1.0).astype(jnp.float32) / jnp.sqrt(jnp.float32(D))
    sample = jax.random.normal(jax.random.fold_in(plant_key, 2), (KVH, HD), jnp.float32)
    unit_heads = sample / jnp.sqrt(jnp.sum(sample * sample, axis=1, keepdims=True) / HD)
    factor = jax.random.uniform(jax.random.fold_in(plant_key, 3), (KVH,), jnp.float32, 0.75, 1.0)
    strength = jnp.sqrt(280.0 / (D * jnp.sqrt(jnp.float32(HD))))
    return (direction, unit_heads * (strength * factor)[:, None])


def draw_doc_blocks(key, part):
    return layout_draw(key)[0]


def draw_plan(key, part):
    return layout_draw(key)[1]


def draw_q_weight(key, part):
    direction, planted = plant_parts(key)
    sample = jnp.clip(jax.random.normal(jax.random.fold_in(key, 41), (D, QH * HD), jnp.float32), -4.0, 4.0)
    per_head = jnp.repeat(planted, QH // KVH, axis=0).reshape(QH * HD)
    result = sample / jnp.sqrt(jnp.float32(D)) + direction[:, None] * per_head[None, :]
    return result.astype(jnp.bfloat16)


def draw_kv_weight(key, part):
    direction, planted = plant_parts(key)
    key_part = jnp.clip(jax.random.normal(jax.random.fold_in(key, 43), (KVH, D, HD), jnp.float32), -4.0, 4.0)
    key_part = key_part / jnp.sqrt(jnp.float32(D)) + direction[None, :, None] * planted[:, None, :]
    value_raw = jnp.clip(jax.random.normal(jax.random.fold_in(key, 47), (KVH, D, HD), jnp.float32), -4.0, 4.0)
    value_raw = value_raw / jnp.sqrt(jnp.float32(D))
    along = jnp.einsum('d,cde->ce', direction, value_raw)
    value_part = value_raw - direction[None, :, None] * along[:, None, :]
    return jnp.concatenate([key_part, value_part], axis=2).astype(jnp.bfloat16)


def draw_y_second(key, part):
    stream_key = jax.random.fold_in(key, 23)
    counts, placed = layout_draw(key)
    direction, planted = plant_parts(key)
    signs = direction * jnp.sqrt(jnp.float32(D))
    starts = (jnp.cumsum(counts) - counts).astype(jnp.int32)
    block_index = jnp.arange(BLOCKS, dtype=jnp.int32)
    leading = jnp.sum(((starts[None, :] == block_index[:, None]) & (counts[None, :] == 2)).astype(jnp.int32), axis=1)
    spacing = BLOCK // 4
    offset = jax.random.randint(jax.random.fold_in(stream_key, 1), (BLOCKS,), 0, spacing).astype(jnp.int32)
    within = jnp.arange(BLOCK, dtype=jnp.int32)
    chosen = (within[None, :] % spacing == offset[:, None]) & (leading[:, None] == 1)
    strength = jnp.exp(jax.random.uniform(jax.random.fold_in(stream_key, 2), (BLOCKS,), jnp.float32, jnp.log(2.5), jnp.log(5.0)))
    noise = jnp.clip(jax.random.normal(jax.random.fold_in(stream_key, 3), (BLOCKS * BLOCK, D), jnp.float32), -4.0, 4.0)
    common = noise
    planted_rows = jnp.repeat(strength, BLOCK)[:, None] * signs[None, :] + noise
    result = jnp.where(chosen.reshape(BLOCKS * BLOCK)[:, None], planted_rows, common)
    return result.astype(jnp.bfloat16)


def plant(values, own_key, smallest, largest):
    shape = values.shape
    index_at = [jax.random.randint(jax.random.fold_in(own_key, axis), (), 0, shape[axis]) for axis in range(len(shape))]
    values = values.at[tuple(index_at)].set(smallest)
    longest = shape.index(max(shape))
    index_at[longest] = (index_at[longest] + 1) % shape[longest]
    return values.at[tuple(index_at)].set(largest)


def block_levels(key, shape, pieces, low, largest):
    def one(position, blocks):
        steps = jax.random.uniform(jax.random.fold_in(jax.random.fold_in(key, 6), position), (blocks,), jnp.float32, low / len(pieces), largest / len(pieces))
        return jnp.repeat(jnp.exp(steps), shape[position] // blocks).reshape((-1,) + (1,) * (len(shape) - position - 1))

    loudness = one(*pieces[0])
    for cut in pieces[1:]:
        loudness = loudness * one(*cut)
    return loudness


def normal_values(own_key, shape, width, most, shards=(), held_as=jnp.bfloat16):
    factor_of = block_levels(own_key, shape, shards, -0.22, 0.18) if shards else 1.0
    values = jax.random.normal(own_key, shape, jnp.float32) * width * factor_of
    return jnp.minimum(jnp.maximum(values, -most), most).astype(held_as)


def setup_inputs(seed: int = 0) -> dict:
    splits = jax.random.split(jax.random.key(seed), 13)
    y_first = normal_values(splits[0], (TOKENS, D), 1.0, 6.0, ((0, 128), (1, 4)))
    y_second = draw_y_second(jax.random.fold_in(splits[12], 71), 0)
    grad_first = normal_values(splits[2], (TOKENS, D), 1.0, 6.0, ((0, 128), (1, 4)))
    grad_second = normal_values(splits[3], (TOKENS, D), 1.0, 6.0, ((0, 128), (1, 4)))
    doc_blocks = draw_doc_blocks(jax.random.fold_in(splits[12], 71), 0)
    last_fill = plant(jax.random.randint(splits[5], (DOCS,), 1, BLOCK + 1), jax.random.fold_in(splits[5], 1), 1, BLOCK).astype(jnp.int32)
    plan = draw_plan(jax.random.fold_in(splits[12], 71), 0)
    q_weight = draw_q_weight(jax.random.fold_in(splits[12], 71), 0)
    kv_weight = draw_kv_weight(jax.random.fold_in(splits[12], 71), 0)
    out_weight = normal_values(splits[9], (QH * HD, D), (QH * HD) ** -0.5, 0.25, ((0, 4),))
    gate_up = normal_values(splits[10], (2, D, FFW), D ** -0.5, 0.1875, ((2, 4),))
    down_weight = normal_values(splits[11], (FFW, D), FFW ** -0.5, 0.125, ((0, 4),))
    return dict(y_first=y_first, y_second=y_second, grad_first=grad_first, grad_second=grad_second, doc_blocks=doc_blocks, last_fill=last_fill, plan=plan, q_weight=q_weight, kv_weight=kv_weight, out_weight=out_weight, gate_up=gate_up, down_weight=down_weight)


EPSILON = 1e-06

def normalize(values):
    inverse = lax.rsqrt(lax.optimization_barrier(jnp.mean(values * values, axis=-1, keepdims=True)) + EPSILON)
    return (values * inverse, inverse)

def norm_back(cotangent, normed, inverse):
    inner = lax.optimization_barrier(jnp.mean(cotangent * normed, axis=-1, keepdims=True))
    return (cotangent - normed * inner) * inverse

def block_table(doc_blocks, last_fill, block_count):
    doc_count = doc_blocks.shape[0]
    starts = (jnp.cumsum(doc_blocks) - doc_blocks).astype(jnp.int32)
    index = jnp.arange(block_count, dtype=jnp.int32)
    owner_doc = (lax.optimization_barrier(jnp.sum((starts[None, :] <= index[:, None]).astype(jnp.int32), axis=1)) - 1).astype(jnp.int32)
    onehot = (owner_doc[:, None] == jnp.arange(doc_count, dtype=jnp.int32)[None, :]).astype(jnp.int32)
    first_block = lax.optimization_barrier(jnp.sum(onehot * starts[None, :], axis=1)).astype(jnp.int32)
    length = lax.optimization_barrier(jnp.sum(onehot * doc_blocks[None, :], axis=1)).astype(jnp.int32)
    filled = lax.optimization_barrier(jnp.sum(onehot * last_fill[None, :], axis=1)).astype(jnp.int32)
    limit = jnp.where(index - first_block == length - 1, filled, BLOCK).astype(jnp.int32)
    return (owner_doc, limit)

def attend_mask(doc_rows, valid_rows):
    count = doc_rows.shape[-1]
    order = jnp.arange(count, dtype=jnp.int32)
    causal = order[None, :] <= order[:, None]
    same_doc = doc_rows[..., :, None] == doc_rows[..., None, :]
    keep = valid_rows[..., None, :] | (order[None, :] == order[:, None])
    return same_doc & causal & keep

def masked_softmax(scores, allowed):
    scores = jnp.where(allowed, scores, -1e+30)
    highest = lax.optimization_barrier(jnp.max(scores, axis=-1, keepdims=True))
    expo = jnp.exp(scores - highest)
    return expo / lax.optimization_barrier(jnp.sum(expo, axis=-1, keepdims=True))

def reference(y_first, y_second, grad_first, grad_second, doc_blocks, last_fill, plan, q_weight, kv_weight, out_weight, gate_up, down_weight):
    f32 = jnp.float32
    bf16 = jnp.bfloat16
    block_count = plan.shape[0]
    order = jnp.arange(block_count, dtype=jnp.int32)
    source = jnp.zeros((block_count,), jnp.int32).at[plan].set(order)
    owner_doc, limit = block_table(doc_blocks, last_fill, block_count)
    pair_rows = 2 * BLOCK
    group_count = block_count // 2

    def arrange(values):
        return values.reshape(block_count, BLOCK, D)[source].reshape(group_count, pair_rows, D)
    row_doc = jnp.repeat(owner_doc[source], BLOCK).reshape(group_count, pair_rows)
    row_limit = jnp.repeat(limit[source], BLOCK).reshape(group_count, pair_rows)
    within = jnp.tile(jnp.arange(BLOCK, dtype=jnp.int32), block_count).reshape(group_count, pair_rows)
    valid = within < row_limit
    scale = 1.0 / math.sqrt(HD)
    per_group = QH // KVH

    def step_group(carry, inputs):
        q_acc, kv_acc, out_acc = carry
        first, second, cot_first, cot_second, docs, live = inputs
        n_one, r_one = normalize(first.astype(f32))
        n_one_b = n_one.astype(bf16)
        gate_pre = jnp.dot(n_one_b, gate_up[0], preferred_element_type=f32)
        up_pre = jnp.dot(n_one_b, gate_up[1], preferred_element_type=f32)
        sigma = jax.nn.sigmoid(gate_pre)
        silu_gate = gate_pre * sigma
        hidden = (silu_gate * up_pre).astype(bf16)
        mixed = jnp.dot(hidden, down_weight, preferred_element_type=f32)
        second_in = (second.astype(f32) - mixed).astype(bf16)
        d_hidden = jnp.dot(cot_second, down_weight.T, preferred_element_type=f32)
        d_gate = (d_hidden * up_pre * sigma * (1.0 + gate_pre * (1.0 - sigma))).astype(bf16)
        d_up = (d_hidden * silu_gate).astype(bf16)
        d_norm_one = jnp.dot(d_gate, gate_up[0].T, preferred_element_type=f32) + jnp.dot(d_up, gate_up[1].T, preferred_element_type=f32)
        first_cot = (cot_first.astype(f32) + norm_back(d_norm_one, n_one, r_one)).astype(bf16)
        n_two, r_two = normalize(second_in.astype(f32))
        n_two_b = n_two.astype(bf16)
        query = jnp.dot(n_two_b, q_weight, preferred_element_type=f32).astype(bf16).reshape(pair_rows, QH, HD)
        keyval = jnp.einsum('sk,ckd->scd', n_two_b.astype(f32), kv_weight.astype(f32)).astype(bf16)
        keys = jnp.repeat(keyval[:, :, :HD], per_group, axis=1)
        values = jnp.repeat(keyval[:, :, HD:], per_group, axis=1)
        allowed = attend_mask(docs, live)
        scores = jnp.einsum('ihd,jhd->hij', query.astype(f32), keys.astype(f32)) * scale
        probs = masked_softmax(scores, allowed[None])
        probs_b = probs.astype(bf16)
        heads_out = jnp.einsum('hij,jhd->ihd', probs_b.astype(f32), values.astype(f32)).astype(bf16).reshape(pair_rows, QH * HD)
        attn = jnp.dot(heads_out, out_weight, preferred_element_type=f32)
        first_in = (first.astype(f32) - live[:, None].astype(f32) * attn).astype(bf16)
        masked_cot = first_cot * live[:, None].astype(bf16)
        out_acc = out_acc + jnp.dot(heads_out.T, masked_cot, preferred_element_type=f32)
        d_out = jnp.dot(masked_cot, out_weight.T, preferred_element_type=f32).astype(bf16).reshape(pair_rows, QH, HD)
        d_prob = jnp.einsum('ihd,jhd->hij', d_out.astype(f32), values.astype(f32))
        delta = lax.optimization_barrier(jnp.sum(probs * d_prob, axis=-1, keepdims=True))
        d_score = (probs * (d_prob - delta) * scale).astype(bf16)
        d_query = jnp.einsum('hij,jhd->ihd', d_score.astype(f32), keys.astype(f32)).astype(bf16).reshape(pair_rows, QH * HD)
        d_key = jnp.einsum('hij,ihd->jhd', d_score.astype(f32), query.astype(f32)).astype(bf16).reshape(pair_rows, KVH, per_group, HD)
        d_value = jnp.einsum('hij,ihd->jhd', probs_b.astype(f32), d_out.astype(f32)).astype(bf16).reshape(pair_rows, KVH, per_group, HD)
        q_acc = q_acc + jnp.dot(n_two_b.T, d_query, preferred_element_type=f32)
        key_grad = jnp.einsum('sk,scpd->ckd', n_two_b.astype(f32), d_key.astype(f32))
        value_grad = jnp.einsum('sk,scpd->ckd', n_two_b.astype(f32), d_value.astype(f32))
        kv_acc = kv_acc + jnp.concatenate([key_grad, value_grad], axis=2)
        d_norm_two = jnp.dot(d_query, q_weight.T, preferred_element_type=f32)
        d_norm_two = d_norm_two + jnp.einsum('scpd,ckd->sk', d_key.astype(f32), kv_weight[:, :, :HD].astype(f32))
        d_norm_two = d_norm_two + jnp.einsum('scpd,ckd->sk', d_value.astype(f32), kv_weight[:, :, HD:].astype(f32))
        second_cot = (cot_second.astype(f32) + norm_back(d_norm_two, n_two, r_two)).astype(bf16)
        return ((q_acc, kv_acc, out_acc), (first_in, second_in, first_cot, second_cot))
    start = (jnp.zeros((D, QH * HD), f32), jnp.zeros((KVH, D, 2 * HD), f32), jnp.zeros((QH * HD, D), f32))
    inputs = (arrange(y_first), arrange(y_second), arrange(grad_first), arrange(grad_second), row_doc, valid)
    grads, results = lax.scan(step_group, start, inputs)
    first_in, second_in, first_cot, second_cot = results
    return (first_in.reshape(TOKENS, D), second_in.reshape(TOKENS, D), first_cot.reshape(TOKENS, D), second_cot.reshape(TOKENS, D), grads[0], grads[1], grads[2])
```

```python
import jax
import jax.numpy as jnp
from jax import lax
from jax.experimental import pallas as pl
from jax.experimental.pallas import tpu as pltpu
from jax.sharding import Mesh
from jax.sharding import PartitionSpec as P

BLOCK = 128
SEQ = ("seq_0", "seq_1", "seq_2")
EPSILON = 1e-06
MP = 4
INTERPRET = False
F32 = jnp.float32
BF16 = jnp.bfloat16


def exchange(value, axis):
    return lax.all_to_all(value, axis, split_axis=0, concat_axis=0, tiled=True)


def dot(left, right, dims):
    return lax.dot_general(left, right, (dims, ((), ())), preferred_element_type=F32)


NN = ((1,), (0,))
NT = ((1,), (1,))
TN = ((0,), (0,))


def slot_facts(doc_blocks, last_fill, plan, slots):
    blocks = plan.shape[0]
    index = jnp.arange(blocks, dtype=jnp.int32)
    mine = jnp.sum(jnp.where(plan[None, :] == slots[:, None], index[None, :], 0), axis=1)
    docs = doc_blocks.shape[0]
    order = jnp.arange(docs, dtype=jnp.int32)
    ends = jnp.sum(jnp.where(order[None, :] <= order[:, None], doc_blocks[None, :], 0), axis=1)
    starts = ends - doc_blocks
    inside = (starts[None, :] <= mine[:, None]) & (mine[:, None] < ends[None, :])
    owner = jnp.sum(jnp.where(inside, order[None, :], 0), axis=1)
    last = inside & (ends[None, :] - 1 == mine[:, None])
    limit = jnp.where(
        jnp.any(last, axis=1), jnp.sum(jnp.where(last, last_fill[None, :], 0), axis=1), BLOCK
    )
    same = (owner[0] == owner[1]).astype(jnp.int32)
    return jnp.stack([limit[0], limit[1], same, same]).astype(jnp.int32)


def feed_forward_kernel(rows_ref, gate_up_ref, down_ref, out_ref, inverse_ref):
    parts, _, lanes = rows_ref.shape
    width = lanes // 2
    total = None
    for m in range(parts):
        piece = rows_ref[m, :, :width].astype(F32)
        part = jnp.sum(piece * piece, axis=-1, keepdims=True)
        total = part if total is None else total + part
    inverse = lax.rsqrt(total / (parts * width) + EPSILON)
    inverse_ref[...] = inverse
    gate = up = dh = 0.0
    for m in range(parts):
        normed = (rows_ref[m, :, :width].astype(F32) * inverse).astype(BF16)
        at = slice(m * width, (m + 1) * width)
        gate += dot(normed, gate_up_ref[0, at, :], NN)
        up += dot(normed, gate_up_ref[1, at, :], NN)
        dh += dot(rows_ref[m, :, width:], down_ref[m], NT)
    sigma = jax.nn.sigmoid(gate)
    silu = gate * sigma
    hidden = (silu * up).astype(BF16)
    d_gate = (dh * up * sigma * (1.0 + gate * (1.0 - sigma))).astype(BF16)
    d_up = (dh * silu).astype(BF16)
    inner = jnp.sum(d_gate.astype(F32) * gate + d_up.astype(F32) * up, axis=-1, keepdims=True)
    inner = inner / (parts * width)
    spare = out_ref.shape[2] // 2
    tail = jnp.broadcast_to(inner, (inner.shape[0], spare - width)).astype(BF16)
    for m in range(parts):
        at = slice(m * width, (m + 1) * width)
        out_ref[m, :, :width] = dot(hidden, down_ref[m], NN).astype(BF16)
        out_ref[m, :, width:spare] = tail
        out_ref[m, :, spare : spare + width] = (
            dot(d_gate, gate_up_ref[0, at, :], NT) + dot(d_up, gate_up_ref[1, at, :], NT)
        ).astype(BF16)
        out_ref[m, :, spare + width :] = tail


def feed_forward(rows, gate_up, down):
    parts, count, lanes = rows.shape
    return pl.pallas_call(
        feed_forward_kernel,
        out_shape=(
            jax.ShapeDtypeStruct((parts, count, 512), BF16),
            jax.ShapeDtypeStruct((count, 1), F32),
        ),
        interpret=INTERPRET,
        compiler_params=pltpu.CompilerParams(vmem_limit_bytes=48 * 2**20),
        name="feed_forward",
    )(rows, gate_up, down)


def attention_kernel(
    facts_ref, rows_ref, query_ref, keyval_ref, proj_ref, out_ref, grads_ref, inverse_ref
):
    parts, count, lanes = rows_ref.shape
    width = lanes // 2
    total = None
    for m in range(parts):
        piece = rows_ref[m, :, :width].astype(F32)
        part = jnp.sum(piece * piece, axis=-1, keepdims=True)
        total = part if total is None else total + part
    inverse = lax.rsqrt(total / (parts * width) + EPSILON)
    inverse_ref[...] = inverse
    normed = []
    query = keyval = d_out = 0.0
    for m in range(parts):
        at = slice(m * width, (m + 1) * width)
        piece = (rows_ref[m, :, :width].astype(F32) * inverse).astype(BF16)
        normed.append(piece)
        query += dot(piece, query_ref[at, :], NN)
        keyval += dot(piece, keyval_ref[at, :], NN)
        d_out += dot(rows_ref[m, :, width:], proj_ref[m], NT)
    query = query.astype(BF16)
    keyval = keyval.astype(BF16)
    d_out = d_out.astype(BF16)
    half = keyval.shape[1] // 2
    lane = lax.broadcasted_iota(jnp.int32, keyval.shape, 1)
    low = lane < half
    wide = keyval.astype(F32)
    turned = pltpu.roll(wide, half, 1)
    keys = jnp.where(low, wide, turned).astype(BF16)
    values = jnp.where(low, turned, wide).astype(BF16)
    row = lax.broadcasted_iota(jnp.int32, (count, count), 0)
    col = lax.broadcasted_iota(jnp.int32, (count, count), 1)
    limit = jnp.where(col < BLOCK, facts_ref[0], facts_ref[1] + BLOCK)
    together = (facts_ref[2] == 1) | ((row >= BLOCK) == (col >= BLOCK))
    allowed = (col <= row) & together & ((col < limit) | (col == row))
    scale = 1.0 / (half**0.5)
    heads = d_query = d_key = d_value = 0.0
    for h in range(2):
        own = low if h == 0 else jnp.logical_not(low)
        zero = jnp.zeros_like(query)
        scores = dot(jnp.where(own, query, zero), keys, NT) * scale
        scores = jnp.where(allowed, scores, -1e30)
        expo = jnp.exp(scores - jnp.max(scores, axis=-1, keepdims=True))
        probs = expo / jnp.sum(expo, axis=-1, keepdims=True)
        probs_b = probs.astype(BF16)
        heads += jnp.where(own, dot(probs_b, values, NN), 0.0)
        d_prob = dot(jnp.where(own, d_out, zero), values, NT)
        delta = jnp.sum(probs * d_prob, axis=-1, keepdims=True)
        d_score = (probs * (d_prob - delta) * scale).astype(BF16)
        d_query += jnp.where(own, dot(d_score, keys, NN), 0.0)
        d_key += jnp.where(own, dot(d_score, query, TN), 0.0)
        d_value += jnp.where(own, dot(probs_b, d_out, TN), 0.0)
    heads = heads.astype(BF16)
    d_query = d_query.astype(BF16)
    d_key = d_key + pltpu.roll(d_key, half, 1)
    d_value = d_value + pltpu.roll(d_value, half, 1)
    d_keyval = jnp.where(low, d_key, d_value).astype(BF16)
    inner = jnp.sum(
        d_query.astype(F32) * query.astype(F32) + d_keyval.astype(F32) * wide,
        axis=-1,
        keepdims=True,
    ) / (parts * width)
    spare = out_ref.shape[2] // 2
    tail = jnp.broadcast_to(inner, (count, spare - width)).astype(BF16)
    for m in range(parts):
        at = slice(m * width, (m + 1) * width)
        out_ref[m, :, :width] = dot(heads, proj_ref[m], NN).astype(BF16)
        out_ref[m, :, width:spare] = tail
        out_ref[m, :, spare : spare + width] = (
            dot(d_query, query_ref[at, :], NT) + dot(d_keyval, keyval_ref[at, :], NT)
        ).astype(BF16)
        out_ref[m, :, spare + width :] = tail
        grads_ref[0, at, :] = dot(normed[m], d_query, TN).astype(BF16)
        grads_ref[1, at, :] = dot(normed[m], d_keyval, TN).astype(BF16)
        grads_ref[2, at, :] = dot(rows_ref[m, :, width:], heads, TN).astype(BF16)


def attention(facts, rows, query, keyval, proj):
    parts, count, lanes = rows.shape
    smem = pl.BlockSpec(memory_space=pltpu.SMEM)
    vmem = pl.BlockSpec(memory_space=pltpu.VMEM)
    return pl.pallas_call(
        attention_kernel,
        in_specs=[smem, vmem, vmem, vmem, vmem],
        out_shape=(
            jax.ShapeDtypeStruct((parts, count, 512), BF16),
            jax.ShapeDtypeStruct((3, query.shape[0], 128), BF16),
            jax.ShapeDtypeStruct((count, 1), F32),
        ),
        interpret=INTERPRET,
        compiler_params=pltpu.CompilerParams(vmem_limit_bytes=48 * 2**20),
        name="attention",
    )(facts, rows, query, keyval, proj)


def to_slots(streams, plan):
    peers = lax.axis_size(SEQ)
    share = BLOCK // peers
    width = streams[0].shape[1]
    whole = len(streams) * width
    sent = jnp.concatenate(
        [s[t * BLOCK : (t + 1) * BLOCK] for t in range(2) for s in streams], axis=1
    ).reshape(peers, share * 2 * whole)
    held = exchange(sent, SEQ).reshape(peers, share, 2 * whole)
    even = held[:, :, :whole].reshape(peers, share * whole)
    odd = held[:, :, whole:].reshape(peers, share * whole)
    pairs = plan.reshape(peers, 2)
    slot = 2 * jnp.arange(peers, dtype=jnp.int32)[:, None]
    halves = []
    for t in range(2):
        pick_even = (pairs[None, :, 0] == slot + t).astype(BF16)
        pick_odd = (pairs[None, :, 1] == slot + t).astype(BF16)
        picked = jnp.dot(pick_even, even, preferred_element_type=F32) + jnp.dot(
            pick_odd, odd, preferred_element_type=F32
        )
        halves.append(picked.astype(BF16).reshape(peers, share, whole))
    placed = jnp.concatenate(halves, axis=2).reshape(peers, share * 2 * whole)
    owned = exchange(placed, SEQ).reshape(BLOCK, 2 * whole)
    return jnp.concatenate([owned[:, :whole], owned[:, whole:]], axis=0)


def shards(
    y_first,
    y_second,
    grad_first,
    grad_second,
    doc_blocks,
    last_fill,
    plan,
    q_weight,
    kv_weight,
    out_weight,
    gate_up,
    down_weight,
):
    count, width = y_first.shape
    seq_size = lax.axis_size(SEQ)
    me = lax.axis_index("mp")
    slots = lax.axis_index(SEQ) * 2 + jnp.arange(2, dtype=jnp.int32)
    facts = slot_facts(doc_blocks, last_fill, plan, slots)
    row = jnp.arange(count, dtype=jnp.int32)
    row_limit = jnp.where(row < BLOCK, facts[0], facts[1] + BLOCK)
    live = (row < row_limit)[:, None]

    groups = kv_weight.shape[0]
    per = MP // groups
    keyval = exchange(jnp.repeat(kv_weight, per, axis=0), "mp").reshape(MP * width, -1)
    down = jnp.moveaxis(down_weight.reshape(-1, MP, width), 1, 0)
    proj = jnp.moveaxis(out_weight.reshape(-1, MP, width), 1, 0)

    moved = to_slots((y_first, grad_second, y_second, grad_first), plan)
    first = moved[:, :width].astype(F32)
    cot_second = moved[:, width : 2 * width].astype(F32)
    second = moved[:, 2 * width : 3 * width].astype(F32)
    cot_first = moved[:, 3 * width :].astype(F32)

    rows = lax.all_gather(moved[:, : 2 * width], "mp", axis=0)
    parts, r_one = feed_forward(rows, gate_up, down)
    arrived = jnp.sum(exchange(parts, "mp").astype(F32), axis=0)
    mixed = arrived[:, :width]
    inner = arrived[:, width : width + 1]
    d_norm = arrived[:, 256 : 256 + width]
    second_in = (second - mixed).astype(BF16)
    first_cot = (cot_first + (d_norm - first * r_one * inner) * r_one).astype(BF16)
    masked = jnp.where(live, first_cot, jnp.zeros_like(first_cot))

    rows = lax.all_gather(jnp.concatenate([second_in, masked], axis=1), "mp", axis=0)
    parts, grads, r_two = attention(facts, rows, q_weight, keyval, proj)
    sent = jnp.moveaxis(grads.reshape(3, seq_size, -1), 0, 1).reshape(seq_size, -1)
    summed = jnp.sum(exchange(sent, SEQ).astype(F32), axis=0).reshape(3, -1, 128)
    arrived = jnp.sum(exchange(parts, "mp").astype(F32), axis=0)
    attn = arrived[:, :width]
    inner = arrived[:, width : width + 1]
    d_norm = arrived[:, 256 : 256 + width]
    first_in = (first - jnp.where(live, attn, 0.0)).astype(BF16)
    normed = second_in.astype(F32) * r_two
    second_cot = (cot_second + (d_norm - normed * inner) * r_two).astype(BF16)

    shares = exchange(jnp.broadcast_to(summed[1], (MP, *summed[1].shape)), "mp")
    kv_grad = shares.reshape(groups, per, *summed[1].shape).sum(axis=1)
    return (
        first_in,
        second_in,
        first_cot,
        second_cot,
        summed[0],
        kv_grad,
        summed[2].T,
    )


def solution(mesh):
    if "seq" in mesh.shape and mesh.shape["seq"] == 128:
        shape = (8, 8, 2, MP)
    else:
        shape = (2, 2, 2, MP)
    finer = Mesh(mesh.devices.reshape(shape), ("seq_0", "seq_1", "seq_2", "mp"))
    return jax.shard_map(
        shards,
        mesh=finer,
        in_specs=(
            P(SEQ, "mp"),
            P(SEQ, "mp"),
            P(SEQ, "mp"),
            P(SEQ, "mp"),
            P(),
            P(),
            P(),
            P(None, "mp"),
            P(None, "mp", None),
            P("mp", None),
            P(None, None, "mp"),
            P("mp", None),
        ),
        out_specs=(
            P(SEQ, "mp"),
            P(SEQ, "mp"),
            P(SEQ, "mp"),
            P(SEQ, "mp"),
            P(SEQ, "mp"),
            P(None, SEQ, None),
            P("mp", SEQ),
        ),
        check_vma=False,
    )
```

```python
import jax
import jax.numpy as jnp
from jax import lax
from jax.experimental import pallas as pl
from jax.experimental.pallas import tpu as pltpu
from jax.sharding import Mesh
from jax.sharding import PartitionSpec as P

BLOCK = 128
SEQ = ("seq_0", "seq_1", "seq_2")
EPSILON = 1e-06
MP = 4
INTERPRET = False
F32 = jnp.float32
BF16 = jnp.bfloat16


PAD = 16


def exchange(value, axis):
    return lax.all_to_all(value, axis, split_axis=0, concat_axis=0, tiled=True)


def dot(left, right, dims):
    return lax.dot_general(left, right, (dims, ((), ())), preferred_element_type=F32)


NN = ((1,), (0,))
NT = ((1,), (1,))
TN = ((0,), (0,))


def slot_facts(doc_blocks, last_fill, plan, slots):
    blocks = plan.shape[0]
    index = jnp.arange(blocks, dtype=jnp.int32)
    mine = jnp.sum(jnp.where(plan[None, :] == slots[:, None], index[None, :], 0), axis=1)
    docs = doc_blocks.shape[0]
    order = jnp.arange(docs, dtype=jnp.int32)
    ends = jnp.sum(jnp.where(order[None, :] <= order[:, None], doc_blocks[None, :], 0), axis=1)
    starts = ends - doc_blocks
    inside = (starts[None, :] <= mine[:, None]) & (mine[:, None] < ends[None, :])
    owner = jnp.sum(jnp.where(inside, order[None, :], 0), axis=1)
    last = inside & (ends[None, :] - 1 == mine[:, None])
    limit = jnp.where(
        jnp.any(last, axis=1), jnp.sum(jnp.where(last, last_fill[None, :], 0), axis=1), BLOCK
    )
    same = (owner[0] == owner[1]).astype(jnp.int32)
    return jnp.stack([limit[0], limit[1], same, lax.axis_index("mp")]).astype(jnp.int32)


def call(kernel, out_shape, *args, scratch=(), smem=0, name=None):
    specs = [pl.BlockSpec(memory_space=pltpu.SMEM)] * smem
    specs += [pl.BlockSpec(memory_space=pltpu.VMEM)] * (len(args) - smem)
    return pl.pallas_call(
        kernel,
        in_specs=specs,
        out_shape=out_shape,
        scratch_shapes=scratch,
        interpret=INTERPRET,
        compiler_params=pltpu.CompilerParams(vmem_limit_bytes=48 * 2**20),
        name=name,
    )(*args)


def put(ref, at, values):
    for j in range(ref.shape[0]):
        ref[pl.ds(j, 1), at, :] = values[None, :, j * 128 : (j + 1) * 128]


def get(ref, at):
    return jnp.concatenate([ref[pl.ds(j, 1), at, :][0] for j in range(ref.shape[0])], axis=1)


def pack_kernel(*refs):
    *streams, out_ref, rows_ref = refs
    for k, stream in enumerate(streams):
        width, count = stream.shape
        gap = jnp.zeros((out_ref.shape[1] - width, count), F32)
        rows = jnp.concatenate([stream[...].astype(F32), gap], axis=0).T
        for t in range(2):
            at = pl.ds(4 * t + k, BLOCK, stride=8)
            put(rows_ref, at, rows[t * BLOCK : (t + 1) * BLOCK])
    out_ref[...] = get(rows_ref, slice(None)).astype(BF16)


def reorder_kernel(plan_ref, held_ref, out_ref, rows_ref, next_ref):
    blocks = plan_ref.shape[1]
    slot = lax.broadcasted_iota(jnp.int32, (blocks, blocks), 0)
    pick = (plan_ref[...] == slot).astype(BF16)
    put(rows_ref, slice(None), held_ref[...].astype(F32))
    for k in range(4):
        at = pl.ds(k, blocks, stride=4)
        put(next_ref, at, dot(pick, get(rows_ref, at).astype(BF16), NN))
    out_ref[...] = get(next_ref, slice(None)).astype(BF16)


def unpack_kernel(rows_in_ref, send_ref, kept_ref, rows_ref):
    width = kept_ref.shape[0] // 4
    put(rows_ref, slice(None), rows_in_ref[...].astype(F32))
    for k in range(4):
        halves = [get(rows_ref, pl.ds(4 * t + k, BLOCK, stride=8)).T for t in range(2)]
        stream = jnp.concatenate(halves, axis=1)[:width].astype(BF16)
        at = slice(k * width, (k + 1) * width)
        kept_ref[at, :] = stream
        if k < 2:
            for m in range(MP):
                send_ref[m, at, :] = stream


def to_slots(streams, plan):
    peers = lax.axis_size(SEQ)
    share = BLOCK // peers
    width = streams[0].shape[0]
    lanes = -(-width // 128) * 128
    rows = 8 * BLOCK
    shape = jax.ShapeDtypeStruct((rows, lanes), BF16)
    scratch = pltpu.VMEM((lanes // 128, rows, 128), F32)
    sent = call(pack_kernel, shape, *streams, scratch=[scratch], name="pack")
    with jax.named_scope("hop_one"):
        held = exchange(sent.reshape(peers, share * 8, lanes), SEQ)
    held = held.reshape(peers, share, 8, lanes)
    placed = []
    for r in range(share):
        placed.append(
            call(
                reorder_kernel,
                jax.ShapeDtypeStruct((peers * 8, lanes), BF16),
                plan.reshape(1, -1),
                held[:, r].reshape(peers * 8, lanes),
                scratch=[pltpu.VMEM((lanes // 128, peers * 8, 128), F32)] * 2,
                name="reorder",
            ).reshape(peers, 8, lanes)
        )
    placed = placed[0] if share == 1 else jnp.stack(placed, axis=1).reshape(peers, -1, lanes)
    with jax.named_scope("hop_two"):
        owned = exchange(placed, SEQ)
    return call(
        unpack_kernel,
        (
            jax.ShapeDtypeStruct((MP, 2 * width, 2 * BLOCK), BF16),
            jax.ShapeDtypeStruct((4 * width, 2 * BLOCK), BF16),
        ),
        owned.reshape(rows, lanes),
        scratch=[scratch],
        name="unpack",
    )


def assemble(rows_ref, whole_ref, first):
    parts, both, _ = rows_ref.shape
    width = both // 2
    for m in range(parts):
        whole_ref[m * width : (m + 1) * width, :] = rows_ref[m, first : first + width, :]


def normalized(whole_ref):
    values = whole_ref[...].astype(F32)
    inverse = lax.rsqrt(jnp.mean(values * values, axis=0, keepdims=True) + EPSILON)
    return (values * inverse).astype(BF16), inverse


def row_sums(values, width):
    ones = jnp.ones((PAD, values.shape[1]), F32)
    sums = lax.dot_general(
        ones, values, (NT, ((), ())), preferred_element_type=F32, precision=lax.Precision.HIGHEST
    )
    return (sums / width).astype(BF16)


def feed_forward_kernel(
    rows_ref, gate_up_ref, down_ref, out_ref, inverse_ref, first_ref, second_ref
):
    parts, both, count = rows_ref.shape
    width = both // 2
    assemble(rows_ref, first_ref, 0)
    assemble(rows_ref, second_ref, width)
    normed, inverse_ref[...] = normalized(first_ref)
    normed = normed.T
    gate = dot(normed, gate_up_ref[0], NN)
    up = dot(normed, gate_up_ref[1], NN)
    dh = dot(second_ref[...].T, down_ref[...], NT)
    sigma = jax.nn.sigmoid(gate)
    silu = gate * sigma
    hidden = (silu * up).astype(BF16)
    d_gate = (dh * up * sigma * (1.0 + gate * (1.0 - sigma))).astype(BF16)
    d_up = (dh * silu).astype(BF16)
    inner = row_sums(d_gate.astype(F32) * gate + d_up.astype(F32) * up, parts * width)
    mixed = dot(hidden, down_ref[...], NN).astype(BF16).T
    for m in range(parts):
        at = slice(m * width, (m + 1) * width)
        out_ref[m, :width, :] = mixed[at]
        out_ref[m, width:both, :] = (
            dot(gate_up_ref[0, at, :], d_gate, NT) + dot(gate_up_ref[1, at, :], d_up, NT)
        ).astype(BF16)
        out_ref[m, both:, :] = inner


def live_columns(facts_ref, shape):
    column = lax.broadcasted_iota(jnp.int32, shape, 1)
    return column < jnp.where(column < BLOCK, facts_ref[0], facts_ref[1] + BLOCK)


def middle_kernel(
    facts_ref, parts_ref, kept_ref, inverse_ref, second_ref, first_cot_ref, send_ref
):
    parts, rows, count = parts_ref.shape
    width = (rows - PAD) // 2
    total = parts_ref[0].astype(F32)
    for m in range(1, parts):
        total += parts_ref[m].astype(F32)
    inverse = inverse_ref[...]
    first = kept_ref[:width, :].astype(F32)
    second = kept_ref[2 * width : 3 * width, :].astype(F32)
    cot = kept_ref[3 * width :, :].astype(F32)
    second = (second - total[:width]).astype(BF16)
    d_norm = total[width : 2 * width]
    inner = total[2 * width : 2 * width + 1]
    cot = (cot + (d_norm - first * inverse * inner) * inverse).astype(BF16)
    second_ref[...] = second
    first_cot_ref[...] = cot
    masked = jnp.where(live_columns(facts_ref, cot.shape), cot.astype(F32), 0.0).astype(BF16)
    for m in range(parts):
        send_ref[m, :width, :] = second
        send_ref[m, width:, :] = masked


def last_kernel(
    facts_ref, *refs
):
    *parts, kept_ref, second_ref, inverse_ref, first_ref, cot_ref = refs
    width = second_ref.shape[0]
    total = parts[0][...].astype(F32)
    for part in parts[1:]:
        total += part[...].astype(F32)
    attn = total[:width]
    d_norm = total[width : 2 * width]
    inner = total[2 * width : 2 * width + 1]
    inverse = inverse_ref[...]
    first = kept_ref[:width, :].astype(F32)
    cot = kept_ref[width : 2 * width, :].astype(F32)
    live = live_columns(facts_ref, attn.shape)
    first_ref[...] = (first - jnp.where(live, attn, 0.0)).astype(BF16)
    normed = second_ref[...].astype(F32) * inverse
    cot_ref[...] = (cot + (d_norm - normed * inner) * inverse).astype(BF16)


def attention_kernel(facts_ref, rows_ref, query_ref, proj_ref, *refs):
    parts, both, count = rows_ref.shape
    width = both // 2
    pieces, refs = refs[:parts], refs[parts:]
    out_refs, refs = refs[:parts], refs[parts:]
    grads_ref, inverse_ref, second_ref, cot_ref, keyval_ref, turned_ref = refs
    me = facts_ref[3]
    for k in range(parts):
        keyval_ref[(me + parts - k) % parts] = pieces[k][...]
    assemble(rows_ref, second_ref, 0)
    assemble(rows_ref, cot_ref, width)
    normed, inverse_ref[...] = normalized(second_ref)
    turned = normed.T
    whole = keyval_ref[...].reshape(parts * width, -1)
    query = dot(turned, query_ref[...].reshape(parts * width, -1), NN).astype(BF16)
    keyval = dot(turned, whole, NN).astype(BF16)
    d_out = dot(cot_ref[...].T, proj_ref[...], NT).astype(BF16)
    half = keyval.shape[1] // 2
    low = lax.broadcasted_iota(jnp.int32, keyval.shape, 1) < half
    wide = keyval.astype(F32)
    rolled = pltpu.roll(wide, half, 1)
    keys = jnp.where(low, wide, rolled).astype(BF16)
    values = jnp.where(low, rolled, wide).astype(BF16)
    row = lax.broadcasted_iota(jnp.int32, (count, count), 0)
    col = lax.broadcasted_iota(jnp.int32, (count, count), 1)
    together = (facts_ref[2] == 1) | ((row >= BLOCK) == (col >= BLOCK))
    allowed = (col <= row) & together & (live_columns(facts_ref, (count, count)) | (col == row))
    scale = 1.0 / (half**0.5)
    heads = d_query = d_key = d_value = 0.0
    for h in range(2):
        own = low if h == 0 else jnp.logical_not(low)
        zero = jnp.zeros_like(query)
        scores = dot(jnp.where(own, query, zero), keys, NT) * scale
        scores = jnp.where(allowed, scores, -1e30)
        expo = jnp.exp(scores - jnp.max(scores, axis=-1, keepdims=True))
        probs = expo / jnp.sum(expo, axis=-1, keepdims=True)
        probs_b = probs.astype(BF16)
        heads += jnp.where(own, dot(probs_b, values, NN), 0.0)
        d_prob = dot(jnp.where(own, d_out, zero), values, NT)
        delta = jnp.sum(probs * d_prob, axis=-1, keepdims=True)
        d_score = (probs * (d_prob - delta) * scale).astype(BF16)
        d_query += jnp.where(own, dot(d_score, keys, NN), 0.0)
        d_key += jnp.where(own, dot(d_score, query, TN), 0.0)
        d_value += jnp.where(own, dot(probs_b, d_out, TN), 0.0)
    heads = heads.astype(BF16)
    d_query = d_query.astype(BF16)
    d_key = d_key + pltpu.roll(d_key, half, 1)
    d_value = d_value + pltpu.roll(d_value, half, 1)
    d_keyval = jnp.where(low, d_key, d_value).astype(BF16)
    spread = lax.broadcasted_iota(jnp.int32, (8 * width // 7, width), 0)
    source = jnp.where(spread % 8 < 7, 7 * (spread // 8) + spread % 8, -1)
    pick = (lax.broadcasted_iota(jnp.int32, source.shape, 1) == source).astype(BF16)
    for m in range(parts):
        at = slice(m * width, (m + 1) * width)
        to = slice(m * pick.shape[0], (m + 1) * pick.shape[0])
        grads = [dot(normed[at], d_query, NN), dot(normed[at], d_keyval, NN)]
        grads.append(dot(cot_ref[at, :], heads, NN))
        grads = jnp.concatenate(grads, axis=1).astype(BF16)
        grads_ref[to, :] = dot(pick, grads, NN).astype(BF16)
    turned_ref[...] = proj_ref[...].T.reshape(turned_ref.shape)
    inner = row_sums(
        d_query.astype(F32) * query.astype(F32) + d_keyval.astype(F32) * wide, parts * width
    )
    for k in range(parts):
        m = (me + k) % parts
        out_refs[k][:width, :] = dot(turned_ref[m], heads, NT).astype(BF16)
        out_refs[k][width:both, :] = (
            dot(query_ref[m], d_query, NT) + dot(keyval_ref[m], d_keyval, NT)
        ).astype(BF16)
        out_refs[k][both:, :] = inner


def turn(value, by):
    return lax.ppermute(value, "mp", [(i, (i + by) % MP) for i in range(MP)])


def shards(
    y_first,
    y_second,
    grad_first,
    grad_second,
    doc_blocks,
    last_fill,
    plan,
    q_weight,
    kv_weight,
    out_weight,
    gate_up,
    down_weight,
):
    count, width = y_first.shape
    seq_size = lax.axis_size(SEQ)
    me = lax.axis_index("mp")
    slots = lax.axis_index(SEQ) * 2 + jnp.arange(2, dtype=jnp.int32)
    facts = slot_facts(doc_blocks, last_fill, plan, slots)
    groups = kv_weight.shape[0]
    with jax.named_scope("weights"):
        pieces = [kv_weight[me >> 1]]
        for k in range(1, MP):
            pieces.append(turn(kv_weight[((me + k) & 3) >> 1], k))

    send, kept = to_slots((y_first.T, grad_second.T, y_second.T, grad_first.T), plan)
    stream = jax.ShapeDtypeStruct((width, count), BF16)
    line = jax.ShapeDtypeStruct((1, count), F32)
    part = jax.ShapeDtypeStruct((2 * width + PAD, count), BF16)
    with jax.named_scope("gather_one"):
        rows = exchange(send, "mp")
    whole = pltpu.VMEM((MP * width, count), BF16)
    parts, r_one = call(
        feed_forward_kernel,
        (jax.ShapeDtypeStruct((MP, *part.shape), BF16), line),
        rows,
        gate_up,
        down_weight,
        scratch=[whole, whole],
        name="feed_forward",
    )
    with jax.named_scope("sum_one"):
        parts = exchange(parts, "mp")
    second_in, first_cot, send = call(
        middle_kernel,
        (stream, stream, jax.ShapeDtypeStruct((MP, 2 * width, count), BF16)),
        facts,
        parts,
        kept,
        r_one,
        smem=1,
        name="middle",
    )
    with jax.named_scope("gather_two"):
        rows = exchange(send, "mp")
    *parts, grads, r_two = call(
        attention_kernel,
        (*[part] * MP, jax.ShapeDtypeStruct((8 * BLOCK, 384), BF16), line),
        facts,
        rows,
        q_weight.reshape(MP, width, -1),
        out_weight,
        *pieces,
        scratch=[whole, whole] + [pltpu.VMEM((MP, width, 128), BF16)] * 2,
        smem=1,
        name="attention",
    )
    with jax.named_scope("weight_grads"):
        grads = exchange(grads.reshape(seq_size, -1, grads.shape[1]), SEQ)
    with jax.named_scope("last_sum"):
        parts = [parts[0]] + [turn(parts[k], k) for k in range(1, MP)]
    first_in, second_cot = call(
        last_kernel, (stream, stream), facts, *parts, kept, second_in, r_two, smem=1, name="last"
    )
    summed = jnp.sum(grads.astype(F32), axis=0).reshape(-1, 8, grads.shape[2])[:, :7]
    summed = summed.reshape(-1, grads.shape[2])
    own = summed[:, 128:256]
    with jax.named_scope("key_grads"):
        shares = exchange(jnp.broadcast_to(own, (MP, *own.shape)), "mp")
    kv_grad = shares.reshape(groups, MP // groups, *own.shape).sum(axis=1)
    return (
        first_in.T,
        second_in.T,
        first_cot.T,
        second_cot.T,
        summed[:, :128],
        kv_grad,
        summed[:, 256:].T,
    )


def solution(mesh):
    if "seq" in mesh.shape and mesh.shape["seq"] == 128:
        shape = (8, 8, 2, MP)
    else:
        shape = (2, 2, 2, MP)
    finer = Mesh(mesh.devices.reshape(shape), ("seq_0", "seq_1", "seq_2", "mp"))
    return jax.shard_map(
        shards,
        mesh=finer,
        in_specs=(
            P(SEQ, "mp"),
            P(SEQ, "mp"),
            P(SEQ, "mp"),
            P(SEQ, "mp"),
            P(),
            P(),
            P(),
            P(None, "mp"),
            P(None, "mp", None),
            P("mp", None),
            P(None, None, "mp"),
            P("mp", None),
        ),
        out_specs=(
            P(SEQ, "mp"),
            P(SEQ, "mp"),
            P(SEQ, "mp"),
            P(SEQ, "mp"),
            P(SEQ, "mp"),
            P(None, SEQ, None),
            P("mp", SEQ),
        ),
        check_vma=False,
    )
```

```python
import jax
import jax.numpy as jnp
from jax import lax
from jax.experimental import pallas as pl
from jax.experimental.pallas import tpu as pltpu
from jax.sharding import Mesh
from jax.sharding import PartitionSpec as P

BLOCK = 128
SEQ = ("seq_0", "seq_1", "seq_2")
EPSILON = 1e-06
MP = 4
INTERPRET = False
F32 = jnp.float32
BF16 = jnp.bfloat16


PAD = 16


def exchange(value, axis):
    return lax.all_to_all(value, axis, split_axis=0, concat_axis=0, tiled=True)


def dot(left, right, dims):
    return lax.dot_general(left, right, (dims, ((), ())), preferred_element_type=F32)


NN = ((1,), (0,))
NT = ((1,), (1,))
TN = ((0,), (0,))


def slot_facts(doc_blocks, last_fill, plan, slots):
    blocks = plan.shape[0]
    index = jnp.arange(blocks, dtype=jnp.int32)
    mine = jnp.sum(jnp.where(plan[None, :] == slots[:, None], index[None, :], 0), axis=1)
    docs = doc_blocks.shape[0]
    order = jnp.arange(docs, dtype=jnp.int32)
    ends = jnp.sum(jnp.where(order[None, :] <= order[:, None], doc_blocks[None, :], 0), axis=1)
    starts = ends - doc_blocks
    inside = (starts[None, :] <= mine[:, None]) & (mine[:, None] < ends[None, :])
    owner = jnp.sum(jnp.where(inside, order[None, :], 0), axis=1)
    last = inside & (ends[None, :] - 1 == mine[:, None])
    limit = jnp.where(
        jnp.any(last, axis=1), jnp.sum(jnp.where(last, last_fill[None, :], 0), axis=1), BLOCK
    )
    same = (owner[0] == owner[1]).astype(jnp.int32)
    return jnp.stack([limit[0], limit[1], same, lax.axis_index("mp")]).astype(jnp.int32)


def call(kernel, out_shape, *args, scratch=(), smem=0, far=(), far_out=(), mib=16, name=None):
    spaces = [pltpu.SMEM] * smem + [pltpu.VMEM] * (len(args) - smem)
    for i in far:
        spaces[i] = pltpu.HBM
    one = not isinstance(out_shape, tuple)
    outs = [pltpu.VMEM] * (1 if one else len(out_shape))
    for i in far_out:
        outs[i] = pltpu.HBM
    outs = [pl.BlockSpec(memory_space=o) for o in outs]
    return pl.pallas_call(
        kernel,
        in_specs=[pl.BlockSpec(memory_space=s) for s in spaces],
        out_specs=outs[0] if one else tuple(outs),
        out_shape=out_shape,
        scratch_shapes=scratch,
        interpret=INTERPRET,
        compiler_params=pltpu.CompilerParams(vmem_limit_bytes=mib * 2**20),
        name=name,
    )(*args)


def put(ref, at, values):
    for j in range(ref.shape[0]):
        ref[pl.ds(j, 1), at, :] = values[None, :, j * 128 : (j + 1) * 128]


def get(ref, at):
    return jnp.concatenate([ref[pl.ds(j, 1), at, :][0] for j in range(ref.shape[0])], axis=1)


def pack_kernel(streams_ref, out_ref, rows_ref):
    width = streams_ref.shape[0] // 4
    gap = jnp.zeros((out_ref.shape[1] - width, streams_ref.shape[1]), F32)
    for k in range(4):
        stream = streams_ref[k * width : (k + 1) * width, :].astype(F32)
        rows = jnp.concatenate([stream, gap], axis=0).T
        for t in range(2):
            at = pl.ds(4 * t + k, BLOCK, stride=8)
            put(rows_ref, at, rows[t * BLOCK : (t + 1) * BLOCK])
    out_ref[...] = get(rows_ref, slice(None)).astype(BF16)


def reorder_kernel(plan_ref, held_ref, out_ref, rows_ref, next_ref):
    blocks = plan_ref.shape[1]
    slot = lax.broadcasted_iota(jnp.int32, (blocks, blocks), 0)
    pick = (plan_ref[...] == slot).astype(BF16)
    put(rows_ref, slice(None), held_ref[...].astype(F32))
    for k in range(4):
        at = pl.ds(k, blocks, stride=4)
        put(next_ref, at, dot(pick, get(rows_ref, at).astype(BF16), NN))
    out_ref[...] = get(next_ref, slice(None)).astype(BF16)


def unpack_kernel(rows_in_ref, send_ref, kept_ref, rows_ref):
    width = kept_ref.shape[0] // 4
    put(rows_ref, slice(None), rows_in_ref[...].astype(F32))
    for k in range(4):
        halves = [get(rows_ref, pl.ds(4 * t + k, BLOCK, stride=8)).T for t in range(2)]
        stream = jnp.concatenate(halves, axis=1)[:width].astype(BF16)
        at = slice(k * width, (k + 1) * width)
        kept_ref[at, :] = stream
        if k < 2:
            send_ref[at, :] = stream


def to_slots(streams, plan):
    peers = lax.axis_size(SEQ)
    share = BLOCK // peers
    width = streams[0].shape[0]
    lanes = -(-width // 128) * 128
    rows = 8 * BLOCK
    shape = jax.ShapeDtypeStruct((rows, lanes), BF16)
    scratch = pltpu.VMEM((lanes // 128, rows, 128), F32)
    sent = call(
        pack_kernel, shape, jnp.concatenate(streams, axis=0), scratch=[scratch], name="pack"
    )
    with jax.named_scope("hop_one"):
        held = exchange(sent.reshape(peers, share * 8, lanes), SEQ)
    held = held.reshape(peers, share, 8, lanes)
    placed = []
    for r in range(share):
        placed.append(
            call(
                reorder_kernel,
                jax.ShapeDtypeStruct((peers * 8, lanes), BF16),
                plan.reshape(1, -1),
                held[:, r].reshape(peers * 8, lanes),
                scratch=[pltpu.VMEM((lanes // 128, peers * 8, 128), F32)] * 2,
                name="reorder",
            ).reshape(peers, 8, lanes)
        )
    placed = placed[0] if share == 1 else jnp.stack(placed, axis=1).reshape(peers, -1, lanes)
    with jax.named_scope("hop_two"):
        owned = exchange(placed, SEQ)
    return call(
        unpack_kernel,
        (
            jax.ShapeDtypeStruct((2 * width, 2 * BLOCK), BF16),
            jax.ShapeDtypeStruct((4 * width, 2 * BLOCK), BF16),
        ),
        owned.reshape(rows, lanes),
        scratch=[scratch],
        name="unpack",
    )


def assemble(rows_ref, whole_ref, first):
    parts, both, _ = rows_ref.shape
    width = both // 2
    for m in range(parts):
        whole_ref[m * width : (m + 1) * width, :] = rows_ref[m, first : first + width, :]


def normalized(whole_ref):
    values = whole_ref[...].astype(F32)
    inverse = lax.rsqrt(jnp.mean(values * values, axis=0, keepdims=True) + EPSILON)
    return (values * inverse).astype(BF16), inverse


def row_sums(values, width):
    ones = jnp.ones((PAD, values.shape[1]), F32)
    sums = lax.dot_general(
        ones, values, (NT, ((), ())), preferred_element_type=F32, precision=lax.Precision.HIGHEST
    )
    return (sums / width).astype(BF16)


def feed_forward_kernel(
    rows_ref, gate_up_ref, down_ref, out_ref, inverse_ref, first_ref, second_ref
):
    parts, both, count = rows_ref.shape
    width = both // 2
    assemble(rows_ref, first_ref, 0)
    assemble(rows_ref, second_ref, width)
    normed, inverse_ref[...] = normalized(first_ref)
    normed = normed.T
    gate = dot(normed, gate_up_ref[0], NN)
    up = dot(normed, gate_up_ref[1], NN)
    dh = dot(second_ref[...].T, down_ref[...], NT)
    sigma = jax.nn.sigmoid(gate)
    silu = gate * sigma
    hidden = (silu * up).astype(BF16)
    d_gate = (dh * up * sigma * (1.0 + gate * (1.0 - sigma))).astype(BF16)
    d_up = (dh * silu).astype(BF16)
    inner = row_sums(d_gate.astype(F32) * gate + d_up.astype(F32) * up, parts * width)
    mixed = dot(hidden, down_ref[...], NN).astype(BF16).T
    for m in range(parts):
        at = slice(m * width, (m + 1) * width)
        out_ref[m, :width, :] = mixed[at]
        out_ref[m, width:both, :] = (
            dot(gate_up_ref[0, at, :], d_gate, NT) + dot(gate_up_ref[1, at, :], d_up, NT)
        ).astype(BF16)
        out_ref[m, both:, :] = inner


def live_columns(facts_ref, shape):
    column = lax.broadcasted_iota(jnp.int32, shape, 1)
    return column < jnp.where(column < BLOCK, facts_ref[0], facts_ref[1] + BLOCK)


def middle_kernel(
    facts_ref, parts_ref, kept_ref, inverse_ref, second_ref, first_cot_ref, send_ref
):
    parts, rows, count = parts_ref.shape
    width = (rows - PAD) // 2
    total = parts_ref[0].astype(F32)
    for m in range(1, parts):
        total += parts_ref[m].astype(F32)
    inverse = inverse_ref[...]
    first = kept_ref[:width, :].astype(F32)
    second = kept_ref[2 * width : 3 * width, :].astype(F32)
    cot = kept_ref[3 * width :, :].astype(F32)
    second = (second - total[:width]).astype(BF16)
    d_norm = total[width : 2 * width]
    inner = total[2 * width : 2 * width + 1]
    cot = (cot + (d_norm - first * inverse * inner) * inverse).astype(BF16)
    second_ref[...] = second
    first_cot_ref[...] = cot
    masked = jnp.where(live_columns(facts_ref, cot.shape), cot.astype(F32), 0.0).astype(BF16)
    send_ref[:width, :] = second
    send_ref[width:, :] = masked


def last_kernel(
    facts_ref, *refs
):
    *parts, kept_ref, second_ref, inverse_ref, first_ref, cot_ref = refs
    width = second_ref.shape[0]
    total = parts[0][...].astype(F32)
    for part in parts[1:]:
        total += part[...].astype(F32)
    attn = total[:width]
    d_norm = total[width : 2 * width]
    inner = total[2 * width : 2 * width + 1]
    inverse = inverse_ref[...]
    first = kept_ref[:width, :].astype(F32)
    cot = kept_ref[width : 2 * width, :].astype(F32)
    live = live_columns(facts_ref, attn.shape)
    first_ref[...] = (first - jnp.where(live, attn, 0.0)).astype(BF16)
    normed = second_ref[...].astype(F32) * inverse
    cot_ref[...] = (cot + (d_norm - normed * inner) * inverse).astype(BF16)


def attention_kernel(facts_ref, rows_ref, query_ref, proj_ref, *refs):
    parts, both, count = rows_ref.shape
    width = both // 2
    pieces, refs = refs[:parts], refs[parts:]
    out_refs, refs = refs[:parts], refs[parts:]
    far_ref, inverse_ref, second_ref, cot_ref, keyval_ref, turned_ref, grads_ref, sem = refs
    me = facts_ref[3]
    for k in range(parts):
        keyval_ref[(me + parts - k) % parts] = pieces[k][...]
    assemble(rows_ref, second_ref, 0)
    assemble(rows_ref, cot_ref, width)
    normed, inverse_ref[...] = normalized(second_ref)
    turned = normed.T
    whole = keyval_ref[...].reshape(parts * width, -1)
    query = dot(turned, query_ref[...].reshape(parts * width, -1), NN).astype(BF16)
    keyval = dot(turned, whole, NN).astype(BF16)
    d_out = dot(cot_ref[...].T, proj_ref[...], NT).astype(BF16)
    half = keyval.shape[1] // 2
    low = lax.broadcasted_iota(jnp.int32, keyval.shape, 1) < half
    wide = keyval.astype(F32)
    rolled = pltpu.roll(wide, half, 1)
    keys = jnp.where(low, wide, rolled).astype(BF16)
    values = jnp.where(low, rolled, wide).astype(BF16)
    row = lax.broadcasted_iota(jnp.int32, (count, count), 0)
    col = lax.broadcasted_iota(jnp.int32, (count, count), 1)
    together = (facts_ref[2] == 1) | ((row >= BLOCK) == (col >= BLOCK))
    allowed = (col <= row) & together & (live_columns(facts_ref, (count, count)) | (col == row))
    scale = 1.0 / (half**0.5)
    heads = d_query = d_key = d_value = 0.0
    for h in range(2):
        own = low if h == 0 else jnp.logical_not(low)
        zero = jnp.zeros_like(query)
        scores = dot(jnp.where(own, query, zero), keys, NT) * scale
        scores = jnp.where(allowed, scores, -1e30)
        expo = jnp.exp(scores - jnp.max(scores, axis=-1, keepdims=True))
        probs = expo / jnp.sum(expo, axis=-1, keepdims=True)
        probs_b = probs.astype(BF16)
        heads += jnp.where(own, dot(probs_b, values, NN), 0.0)
        d_prob = dot(jnp.where(own, d_out, zero), values, NT)
        delta = jnp.sum(probs * d_prob, axis=-1, keepdims=True)
        d_score = (probs * (d_prob - delta) * scale).astype(BF16)
        d_query += jnp.where(own, dot(d_score, keys, NN), 0.0)
        d_key += jnp.where(own, dot(d_score, query, TN), 0.0)
        d_value += jnp.where(own, dot(probs_b, d_out, TN), 0.0)
    heads = heads.astype(BF16)
    d_query = d_query.astype(BF16)
    d_key = d_key + pltpu.roll(d_key, half, 1)
    d_value = d_value + pltpu.roll(d_value, half, 1)
    d_keyval = jnp.where(low, d_key, d_value).astype(BF16)
    spread = lax.broadcasted_iota(jnp.int32, (8 * width // 7, width), 0)
    source = jnp.where(spread % 8 < 7, 7 * (spread // 8) + spread % 8, -1)
    pick = (lax.broadcasted_iota(jnp.int32, source.shape, 1) == source).astype(BF16)
    for m in range(parts):
        at = slice(m * width, (m + 1) * width)
        to = slice(m * pick.shape[0], (m + 1) * pick.shape[0])
        grads = [dot(normed[at], d_query, NN), dot(normed[at], d_keyval, NN)]
        grads.append(dot(cot_ref[at, :], heads, NN))
        grads = jnp.concatenate(grads, axis=1).astype(BF16)
        grads_ref[to, :] = dot(pick, grads, NN).astype(BF16)
    copy = pltpu.make_async_copy(grads_ref, far_ref, sem)
    copy.start()
    turned_ref[...] = proj_ref[...].T.reshape(turned_ref.shape)
    inner = row_sums(
        d_query.astype(F32) * query.astype(F32) + d_keyval.astype(F32) * wide, parts * width
    )
    for k in range(parts):
        m = (me + k) % parts
        out_refs[k][:width, :] = dot(turned_ref[m], heads, NT).astype(BF16)
        out_refs[k][width:both, :] = (
            dot(query_ref[m], d_query, NT) + dot(keyval_ref[m], d_keyval, NT)
        ).astype(BF16)
        out_refs[k][both:, :] = inner
    copy.wait()


def finish_kernel(grads_ref, query_ref, out_ref, own_ref):
    total = jnp.sum(grads_ref[...].astype(F32), axis=0)
    total = total.reshape(-1, 8, total.shape[1])[:, :7].reshape(-1, total.shape[1])
    query_ref[...] = total[:, :128]
    out_ref[...] = total[:, 256:]
    for m in range(MP):
        own_ref[m] = total[:, 128:256]


def pair_kernel(shares_ref, out_ref):
    groups = out_ref.shape[1]
    per = MP // groups
    for g in range(groups):
        out_ref[:, g, :] = shares_ref[g * per] + shares_ref[g * per + 1]


def turn(value, by):
    return lax.ppermute(value, "mp", [(i, (i + by) % MP) for i in range(MP)])


def shards(
    y_first,
    y_second,
    grad_first,
    grad_second,
    doc_blocks,
    last_fill,
    plan,
    q_weight,
    kv_weight,
    out_weight,
    gate_up,
    down_weight,
):
    count, width = y_first.shape
    seq_size = lax.axis_size(SEQ)
    me = lax.axis_index("mp")
    slots = lax.axis_index(SEQ) * 2 + jnp.arange(2, dtype=jnp.int32)
    facts = slot_facts(doc_blocks, last_fill, plan, slots)
    groups = kv_weight.shape[0]
    with jax.named_scope("weights"):
        pieces = [kv_weight[me >> 1]]
        for k in range(1, MP):
            pieces.append(turn(kv_weight[((me + k) & 3) >> 1], k))

    send, kept = to_slots((y_first.T, grad_second.T, y_second.T, grad_first.T), plan)
    send, facts, pieces = lax.optimization_barrier((send, facts, pieces))
    stream = jax.ShapeDtypeStruct((width, count), BF16)
    line = jax.ShapeDtypeStruct((1, count), F32)
    part = jax.ShapeDtypeStruct((2 * width + PAD, count), BF16)
    with jax.named_scope("gather_one"):
        rows = lax.all_gather(send, "mp", axis=0)
    whole = pltpu.VMEM((MP * width, count), BF16)
    parts, r_one = call(
        feed_forward_kernel,
        (jax.ShapeDtypeStruct((MP, *part.shape), BF16), line),
        rows,
        gate_up,
        down_weight,
        scratch=[whole, whole],
        name="feed_forward",
    )
    with jax.named_scope("sum_one"):
        parts = exchange(parts, "mp")
    second_in, first_cot, send = call(
        middle_kernel,
        (stream, stream, jax.ShapeDtypeStruct((2 * width, count), BF16)),
        facts,
        parts,
        kept,
        r_one,
        smem=1,
        name="middle",
    )
    with jax.named_scope("gather_two"):
        rows = lax.all_gather(send, "mp", axis=0)
    *parts, grads, r_two = call(
        attention_kernel,
        (*[part] * MP, jax.ShapeDtypeStruct((8 * BLOCK, 384), BF16), line),
        facts,
        rows,
        q_weight.reshape(MP, width, -1),
        out_weight,
        *pieces,
        scratch=[
            whole,
            whole,
            *[pltpu.VMEM((MP, width, 128), BF16)] * 2,
            pltpu.VMEM((8 * BLOCK, 384), BF16),
            pltpu.SemaphoreType.DMA,
        ],
        far_out=(MP,),
        smem=1,
        name="attention",
    )
    with jax.named_scope("weight_grads"):
        grads = exchange(grads.reshape(seq_size, -1, grads.shape[1]), SEQ)
    with jax.named_scope("last_sum"):
        parts = [parts[0]] + [turn(parts[k], k) for k in range(1, MP)]
    first_in, second_cot = call(
        last_kernel, (stream, stream), facts, *parts, kept, second_in, r_two, smem=1, name="last"
    )
    share = jax.ShapeDtypeStruct((7 * BLOCK // seq_size, 128), F32)
    query_grad, out_grad, own = call(
        finish_kernel,
        (share, share, jax.ShapeDtypeStruct((MP, *share.shape), F32)),
        grads,
        name="finish",
    )
    with jax.named_scope("key_grads"):
        shares = exchange(own, "mp")
    kv_grad = call(
        pair_kernel,
        jax.ShapeDtypeStruct((shares.shape[1], groups, 128), F32),
        shares,
        name="pair",
    )
    return (
        first_in.T,
        second_in.T,
        first_cot.T,
        second_cot.T,
        query_grad,
        kv_grad.transpose(1, 0, 2),
        out_grad.T,
    )


def solution(mesh):
    if "seq" in mesh.shape and mesh.shape["seq"] == 128:
        shape = (8, 8, 2, MP)
    else:
        shape = (2, 2, 2, MP)
    finer = Mesh(mesh.devices.reshape(shape), ("seq_0", "seq_1", "seq_2", "mp"))
    return jax.shard_map(
        shards,
        mesh=finer,
        in_specs=(
            P(SEQ, "mp"),
            P(SEQ, "mp"),
            P(SEQ, "mp"),
            P(SEQ, "mp"),
            P(),
            P(),
            P(),
            P(None, "mp"),
            P(None, "mp", None),
            P("mp", None),
            P(None, None, "mp"),
            P("mp", None),
        ),
        out_specs=(
            P(SEQ, "mp"),
            P(SEQ, "mp"),
            P(SEQ, "mp"),
            P(SEQ, "mp"),
            P(SEQ, "mp"),
            P(None, SEQ, None),
            P("mp", SEQ),
        ),
        check_vma=False,
    )
```

```python
from functools import partial

import jax
import jax.numpy as jnp
from jax import lax
from jax.experimental import pallas as pl
from jax.experimental.pallas import tpu as pltpu
from jax.sharding import Mesh
from jax.sharding import PartitionSpec as P

BLOCK = 128
SEQ = ("seq_0", "seq_1", "seq_2")
EPSILON = 1e-06
MP = 4
INTERPRET = False
F32 = jnp.float32
BF16 = jnp.bfloat16


PAD = 16


def exchange(value, axis):
    return lax.all_to_all(value, axis, split_axis=0, concat_axis=0, tiled=True)


def dot(left, right, dims):
    return lax.dot_general(left, right, (dims, ((), ())), preferred_element_type=F32)


NN = ((1,), (0,))
NT = ((1,), (1,))
TN = ((0,), (0,))


def slot_facts(doc_blocks, last_fill, plan, slots):
    blocks = plan.shape[0]
    index = jnp.arange(blocks, dtype=jnp.int32)
    mine = jnp.sum(jnp.where(plan[None, :] == slots[:, None], index[None, :], 0), axis=1)
    docs = doc_blocks.shape[0]
    order = jnp.arange(docs, dtype=jnp.int32)
    ends = jnp.sum(jnp.where(order[None, :] <= order[:, None], doc_blocks[None, :], 0), axis=1)
    starts = ends - doc_blocks
    inside = (starts[None, :] <= mine[:, None]) & (mine[:, None] < ends[None, :])
    owner = jnp.sum(jnp.where(inside, order[None, :], 0), axis=1)
    last = inside & (ends[None, :] - 1 == mine[:, None])
    limit = jnp.where(
        jnp.any(last, axis=1), jnp.sum(jnp.where(last, last_fill[None, :], 0), axis=1), BLOCK
    )
    same = (owner[0] == owner[1]).astype(jnp.int32)
    return jnp.stack([limit[0], limit[1], same, lax.axis_index("mp"), lax.axis_index("seq_2")]).astype(
        jnp.int32
    )


def call(kernel, out_shape, *args, scratch=(), smem=0, far=(), far_out=(), mib=16, name=None):
    spaces = [pltpu.SMEM] * smem + [pltpu.VMEM] * (len(args) - smem)
    for i in far:
        spaces[i] = pltpu.HBM
    one = not isinstance(out_shape, tuple)
    outs = [pltpu.VMEM] * (1 if one else len(out_shape))
    for i in far_out:
        outs[i] = pltpu.HBM
    outs = [pl.BlockSpec(memory_space=o) for o in outs]
    return pl.pallas_call(
        kernel,
        in_specs=[pl.BlockSpec(memory_space=s) for s in spaces],
        out_specs=outs[0] if one else tuple(outs),
        out_shape=out_shape,
        scratch_shapes=scratch,
        interpret=INTERPRET,
        compiler_params=pltpu.CompilerParams(vmem_limit_bytes=mib * 2**20),
        name=name,
    )(*args)


def put(ref, at, values):
    for j in range(ref.shape[0]):
        ref[pl.ds(j, 1), at, :] = values[None, :, j * 128 : (j + 1) * 128]


def get(ref, at):
    return jnp.concatenate([ref[pl.ds(j, 1), at, :][0] for j in range(ref.shape[0])], axis=1)


def pack_kernel(streams_ref, out_ref, rows_ref):
    width = streams_ref.shape[0] // 4
    gap = jnp.zeros((out_ref.shape[1] - width, streams_ref.shape[1]), F32)
    for k in range(4):
        stream = streams_ref[k * width : (k + 1) * width, :].astype(F32)
        rows = jnp.concatenate([stream, gap], axis=0).T
        for t in range(2):
            at = pl.ds(4 * t + k, BLOCK, stride=8)
            put(rows_ref, at, rows[t * BLOCK : (t + 1) * BLOCK])
    out_ref[...] = get(rows_ref, slice(None)).astype(BF16)


def reorder_kernel(plan_ref, held_ref, out_ref, rows_ref, next_ref):
    blocks = plan_ref.shape[1]
    slot = lax.broadcasted_iota(jnp.int32, (blocks, blocks), 0)
    pick = (plan_ref[...] == slot).astype(BF16)
    put(rows_ref, slice(None), held_ref[...].astype(F32))
    for k in range(4):
        at = pl.ds(k, blocks, stride=4)
        put(next_ref, at, dot(pick, get(rows_ref, at).astype(BF16), NN))
    out_ref[...] = get(next_ref, slice(None)).astype(BF16)


def unpack_kernel(rows_in_ref, send_ref, kept_ref, rows_ref):
    width = kept_ref.shape[0] // 4
    put(rows_ref, slice(None), rows_in_ref[...].astype(F32))
    for k in range(4):
        halves = [get(rows_ref, pl.ds(4 * t + k, BLOCK, stride=8)).T for t in range(2)]
        stream = jnp.concatenate(halves, axis=1)[:width].astype(BF16)
        at = slice(k * width, (k + 1) * width)
        kept_ref[at, :] = stream
        if k < 2:
            send_ref[at, :] = stream


def turn(value, by):
    return lax.ppermute(value, "mp", [(i, (i + by) % MP) for i in range(MP)])


def to_slots(streams, kv_weight, *tables):
    peers = lax.axis_size(SEQ)
    plan = tables[-1]
    share = BLOCK // peers
    width = streams[0].shape[0]
    lanes = -(-width // 128) * 128
    rows = 8 * BLOCK
    shape = jax.ShapeDtypeStruct((rows, lanes), BF16)
    scratch = pltpu.VMEM((lanes // 128, rows, 128), F32)
    sent = call(
        pack_kernel, shape, jnp.concatenate(streams, axis=0), scratch=[scratch], name="pack"
    )
    with jax.named_scope("hop_one"):
        held = exchange(sent.reshape(peers, share * 8, lanes), SEQ)
    slots = lax.axis_index(SEQ) * 2 + jnp.arange(2, dtype=jnp.int32)
    facts = slot_facts(*tables, slots)
    with jax.named_scope("weights"):
        me = lax.axis_index("mp")
        pieces = [kv_weight[me >> 1]]
        for k in range(1, MP):
            pieces.append(turn(kv_weight[((me + k) & 3) >> 1], k))
    held = held.reshape(peers, share, 8, lanes)
    placed = []
    for r in range(share):
        placed.append(
            call(
                reorder_kernel,
                jax.ShapeDtypeStruct((peers * 8, lanes), BF16),
                plan.reshape(1, -1),
                held[:, r].reshape(peers * 8, lanes),
                scratch=[pltpu.VMEM((lanes // 128, peers * 8, 128), F32)] * 2,
                name="reorder",
            ).reshape(peers, 8, lanes)
        )
    placed = placed[0] if share == 1 else jnp.stack(placed, axis=1).reshape(peers, -1, lanes)
    with jax.named_scope("hop_two"):
        owned = exchange(placed, SEQ)
    return facts, pieces, *call(
        unpack_kernel,
        (
            jax.ShapeDtypeStruct((2 * width, 2 * BLOCK), BF16),
            jax.ShapeDtypeStruct((4 * width, 2 * BLOCK), BF16),
        ),
        owned.reshape(rows, lanes),
        scratch=[scratch],
        name="unpack",
    )


def assemble(rows_ref, whole_ref, first):
    parts, both, _ = rows_ref.shape
    width = both // 2
    for m in range(parts):
        whole_ref[m * width : (m + 1) * width, :] = rows_ref[m, first : first + width, :]


def normalized(whole_ref):
    values = whole_ref[...].astype(F32)
    inverse = lax.rsqrt(jnp.mean(values * values, axis=0, keepdims=True) + EPSILON)
    return (values * inverse).astype(BF16), inverse


def row_sums(values, width):
    ones = jnp.ones((PAD, values.shape[1]), F32)
    sums = lax.dot_general(
        ones, values, (NT, ((), ())), preferred_element_type=F32, precision=lax.Precision.HIGHEST
    )
    return (sums / width).astype(BF16)


def feed_forward_kernel(
    rows_ref, gate_up_ref, down_ref, out_ref, inverse_ref, first_ref, second_ref
):
    parts, both, count = rows_ref.shape
    width = both // 2
    assemble(rows_ref, first_ref, 0)
    assemble(rows_ref, second_ref, width)
    normed, inverse_ref[...] = normalized(first_ref)
    normed = normed.T
    gate = dot(normed, gate_up_ref[0], NN)
    up = dot(normed, gate_up_ref[1], NN)
    dh = dot(second_ref[...].T, down_ref[...], NT)
    sigma = jax.nn.sigmoid(gate)
    silu = gate * sigma
    hidden = (silu * up).astype(BF16)
    d_gate = (dh * up * sigma * (1.0 + gate * (1.0 - sigma))).astype(BF16)
    d_up = (dh * silu).astype(BF16)
    inner = row_sums(d_gate.astype(F32) * gate + d_up.astype(F32) * up, parts * width)
    mixed = dot(hidden, down_ref[...], NN).astype(BF16).T
    for m in range(parts):
        at = slice(m * width, (m + 1) * width)
        out_ref[m, :width, :] = mixed[at]
        out_ref[m, width:both, :] = (
            dot(gate_up_ref[0, at, :], d_gate, NT) + dot(gate_up_ref[1, at, :], d_up, NT)
        ).astype(BF16)
        out_ref[m, both:, :] = inner


def live_columns(facts_ref, shape):
    column = lax.broadcasted_iota(jnp.int32, shape, 1)
    return column < jnp.where(column < BLOCK, facts_ref[0], facts_ref[1] + BLOCK)


def middle_kernel(
    facts_ref, parts_ref, kept_ref, inverse_ref, second_ref, first_cot_ref, send_ref
):
    parts, rows, count = parts_ref.shape
    width = (rows - PAD) // 2
    total = parts_ref[0].astype(F32)
    for m in range(1, parts):
        total += parts_ref[m].astype(F32)
    inverse = inverse_ref[...]
    first = kept_ref[:width, :].astype(F32)
    second = kept_ref[2 * width : 3 * width, :].astype(F32)
    cot = kept_ref[3 * width :, :].astype(F32)
    second = (second - total[:width]).astype(BF16)
    d_norm = total[width : 2 * width]
    inner = total[2 * width : 2 * width + 1]
    cot = (cot + (d_norm - first * inverse * inner) * inverse).astype(BF16)
    second_ref[...] = second
    first_cot_ref[...] = cot
    masked = jnp.where(live_columns(facts_ref, cot.shape), cot.astype(F32), 0.0).astype(BF16)
    send_ref[:width, :] = second
    send_ref[width:, :] = masked


def last_kernel(
    facts_ref, *refs
):
    *parts, kept_ref, second_ref, inverse_ref, first_ref, cot_ref = refs
    width = second_ref.shape[0]
    total = parts[0][...].astype(F32)
    for part in parts[1:]:
        total += part[...].astype(F32)
    attn = total[:width]
    d_norm = total[width : 2 * width]
    inner = total[2 * width : 2 * width + 1]
    inverse = inverse_ref[...]
    first = kept_ref[:width, :].astype(F32)
    cot = kept_ref[width : 2 * width, :].astype(F32)
    live = live_columns(facts_ref, attn.shape)
    first_ref[...] = (first - jnp.where(live, attn, 0.0)).astype(BF16)
    normed = second_ref[...].astype(F32) * inverse
    cot_ref[...] = (cot + (d_norm - normed * inner) * inverse).astype(BF16)


def attention_kernel(groups, facts_ref, rows_ref, query_ref, proj_ref, *refs):
    parts, both, count = rows_ref.shape
    width = both // 2
    pieces, refs = refs[:parts], refs[parts:]
    kept_ref, given_ref, makings_ref, keyval_ref, inner_ref, inverse_ref = refs[:6]
    second_ref, cot_ref, grads_ref = refs[6:]
    me = facts_ref[3]
    for k in range(parts):
        keyval_ref[(me + parts - k) % parts] = pieces[k][...]
    assemble(rows_ref, second_ref, 0)
    assemble(rows_ref, cot_ref, width)
    normed, inverse_ref[...] = normalized(second_ref)
    turned = normed.T
    whole = keyval_ref[...].reshape(parts * width, -1)
    query = dot(turned, query_ref[...].reshape(parts * width, -1), NN).astype(BF16)
    keyval = dot(turned, whole, NN).astype(BF16)
    d_out = dot(cot_ref[...].T, proj_ref[...], NT).astype(BF16)
    half = keyval.shape[1] // 2
    low = lax.broadcasted_iota(jnp.int32, keyval.shape, 1) < half
    wide = keyval.astype(F32)
    rolled = pltpu.roll(wide, half, 1)
    keys = jnp.where(low, wide, rolled).astype(BF16)
    values = jnp.where(low, rolled, wide).astype(BF16)
    row = lax.broadcasted_iota(jnp.int32, (count, count), 0)
    col = lax.broadcasted_iota(jnp.int32, (count, count), 1)
    together = (facts_ref[2] == 1) | ((row >= BLOCK) == (col >= BLOCK))
    allowed = (col <= row) & together & (live_columns(facts_ref, (count, count)) | (col == row))
    scale = 1.0 / (half**0.5)
    heads = d_query = d_key = d_value = 0.0
    for h in range(2):
        own = low if h == 0 else jnp.logical_not(low)
        zero = jnp.zeros_like(query)
        scores = dot(jnp.where(own, query, zero), keys, NT) * scale
        scores = jnp.where(allowed, scores, -1e30)
        expo = jnp.exp(scores - jnp.max(scores, axis=-1, keepdims=True))
        probs = expo / jnp.sum(expo, axis=-1, keepdims=True)
        probs_b = probs.astype(BF16)
        heads += jnp.where(own, dot(probs_b, values, NN), 0.0)
        d_prob = dot(jnp.where(own, d_out, zero), values, NT)
        delta = jnp.sum(probs * d_prob, axis=-1, keepdims=True)
        d_score = (probs * (d_prob - delta) * scale).astype(BF16)
        d_query += jnp.where(own, dot(d_score, keys, NN), 0.0)
        d_key += jnp.where(own, dot(d_score, query, TN), 0.0)
        d_value += jnp.where(own, dot(probs_b, d_out, TN), 0.0)
    heads = heads.astype(BF16)
    d_query = d_query.astype(BF16)
    d_key = d_key + pltpu.roll(d_key, half, 1)
    d_value = d_value + pltpu.roll(d_value, half, 1)
    d_keyval = jnp.where(low, d_key, d_value).astype(BF16)
    makings_ref[0] = heads
    makings_ref[1] = d_query
    makings_ref[2] = d_keyval
    inner_ref[...] = row_sums(
        d_query.astype(F32) * query.astype(F32) + d_keyval.astype(F32) * wide, parts * width
    )
    lines = 8 * width // 7
    spread = lax.broadcasted_iota(jnp.int32, (lines, width), 0)
    core = (spread >= lines // 2).astype(jnp.int32)
    place = (spread - core * (lines // 2)) // 8
    group = (2 * (place // groups) + core) * groups + place % groups
    source = jnp.where(spread % 8 < 7, 7 * group + spread % 8, -1)
    pick = (lax.broadcasted_iota(jnp.int32, source.shape, 1) == source).astype(BF16)
    for m in range(parts):
        at = slice(m * width, (m + 1) * width)
        grads = [dot(normed[at], d_query, NN), dot(normed[at], d_keyval, NN)]
        grads.append(dot(cot_ref[at, :], heads, NN))
        grads = jnp.concatenate(grads, axis=1).astype(BF16)
        grads = dot(pick, grads, NN).astype(BF16)
        to = slice(m * (lines // 2), (m + 1) * (lines // 2))
        for c in range(2):
            grads_ref[c, to, :] = grads[c * (lines // 2) : (c + 1) * (lines // 2)]
    kept_ref[...] = grads_ref[facts_ref[4]]
    given_ref[...] = grads_ref[1 - facts_ref[4]]


def pieces_kernel(
    facts_ref, makings_ref, keyval_ref, inner_ref, query_ref, proj_ref, *refs
):
    parts, width, _ = query_ref.shape
    both = 2 * width
    out_refs, turned_ref = refs[:parts], refs[parts]
    me = facts_ref[3]
    heads, d_query, d_keyval = makings_ref[0], makings_ref[1], makings_ref[2]
    turned_ref[...] = proj_ref[...].T.reshape(turned_ref.shape)
    for k in range(parts):
        m = (me + k) % parts
        out_refs[k][:width, :] = dot(turned_ref[m], heads, NT).astype(BF16)
        out_refs[k][width:both, :] = (
            dot(query_ref[m], d_query, NT) + dot(keyval_ref[m], d_keyval, NT)
        ).astype(BF16)
        out_refs[k][both:, :] = inner_ref[...]


def add_kernel(left_ref, right_ref, out_ref):
    out_ref[...] = (left_ref[...].astype(F32) + right_ref[...].astype(F32)).astype(BF16)


def finish_kernel(grads_ref, query_ref, out_ref, own_ref):
    total = jnp.sum(grads_ref[...].astype(F32), axis=0)
    total = total.reshape(-1, 8, total.shape[1])[:, :7].reshape(-1, total.shape[1])
    query_ref[...] = total[:, :128]
    out_ref[...] = total[:, 256:]
    for m in range(MP):
        own_ref[m] = total[:, 128:256]


def pair_kernel(shares_ref, out_ref):
    groups = out_ref.shape[1]
    per = MP // groups
    for g in range(groups):
        out_ref[:, g, :] = shares_ref[g * per] + shares_ref[g * per + 1]


def shards(
    y_first,
    y_second,
    grad_first,
    grad_second,
    doc_blocks,
    last_fill,
    plan,
    q_weight,
    kv_weight,
    out_weight,
    gate_up,
    down_weight,
):
    count, width = y_first.shape
    seq_size = lax.axis_size(SEQ)
    groups = kv_weight.shape[0]
    streams = (y_first.T, grad_second.T, y_second.T, grad_first.T)
    facts, pieces, send, kept = to_slots(streams, kv_weight, doc_blocks, last_fill, plan)
    send, facts, pieces = lax.optimization_barrier((send, facts, pieces))
    stream = jax.ShapeDtypeStruct((width, count), BF16)
    line = jax.ShapeDtypeStruct((1, count), F32)
    part = jax.ShapeDtypeStruct((2 * width + PAD, count), BF16)
    with jax.named_scope("gather_one"):
        rows = lax.all_gather(send, "mp", axis=0)
    whole = pltpu.VMEM((MP * width, count), BF16)
    parts, r_one = call(
        feed_forward_kernel,
        (jax.ShapeDtypeStruct((MP, *part.shape), BF16), line),
        rows,
        gate_up,
        down_weight,
        scratch=[whole, whole],
        name="feed_forward",
    )
    with jax.named_scope("sum_one"):
        parts = exchange(parts, "mp")
    second_in, first_cot, send = call(
        middle_kernel,
        (stream, stream, jax.ShapeDtypeStruct((2 * width, count), BF16)),
        facts,
        parts,
        kept,
        r_one,
        smem=1,
        name="middle",
    )
    with jax.named_scope("gather_two"):
        rows = lax.all_gather(send, "mp", axis=0)
    query = q_weight.reshape(MP, width, -1)
    half = jax.ShapeDtypeStruct((4 * BLOCK, 384), BF16)
    kept_grads, given, makings, keyval, inner, r_two = call(
        partial(attention_kernel, BLOCK // seq_size),
        (
            half,
            half,
            jax.ShapeDtypeStruct((3, count, 128), BF16),
            jax.ShapeDtypeStruct((MP, width, 128), BF16),
            jax.ShapeDtypeStruct((PAD, count), BF16),
            line,
        ),
        facts,
        rows,
        query,
        out_weight,
        *pieces,
        scratch=[whole, whole, pltpu.VMEM((2, *half.shape), BF16)],
        smem=1,
        name="attention",
    )
    with jax.named_scope("core_sum"):
        given = lax.ppermute(given, "seq_2", [(0, 1), (1, 0)])
    grads = call(add_kernel, half, kept_grads, given, name="add")
    with jax.named_scope("weight_grads"):
        grads = exchange(grads.reshape(seq_size // 2, -1, grads.shape[1]), SEQ[:2])
    parts = call(
        pieces_kernel,
        (part,) * MP,
        facts,
        makings,
        keyval,
        inner,
        query,
        out_weight,
        scratch=[pltpu.VMEM((MP, width, 128), BF16)],
        smem=1,
        name="pieces",
    )
    with jax.named_scope("last_sum"):
        parts = [parts[0]] + [turn(parts[k], k) for k in range(1, MP)]
    first_in, second_cot = call(
        last_kernel, (stream, stream), facts, *parts, kept, second_in, r_two, smem=1, name="last"
    )
    share = jax.ShapeDtypeStruct((7 * BLOCK // seq_size, 128), F32)
    query_grad, out_grad, own = call(
        finish_kernel,
        (share, share, jax.ShapeDtypeStruct((MP, *share.shape), F32)),
        grads,
        name="finish",
    )
    with jax.named_scope("key_grads"):
        shares = exchange(own, "mp")
    kv_grad = call(
        pair_kernel,
        jax.ShapeDtypeStruct((shares.shape[1], groups, 128), F32),
        shares,
        name="pair",
    )
    return (
        first_in.T,
        second_in.T,
        first_cot.T,
        second_cot.T,
        query_grad,
        kv_grad.transpose(1, 0, 2),
        out_grad.T,
    )


def solution(mesh):
    if "seq" in mesh.shape and mesh.shape["seq"] == 128:
        shape = (8, 8, 2, MP)
    else:
        shape = (2, 2, 2, MP)
    finer = Mesh(mesh.devices.reshape(shape), ("seq_0", "seq_1", "seq_2", "mp"))
    return jax.shard_map(
        shards,
        mesh=finer,
        in_specs=(
            P(SEQ, "mp"),
            P(SEQ, "mp"),
            P(SEQ, "mp"),
            P(SEQ, "mp"),
            P(),
            P(),
            P(),
            P(None, "mp"),
            P(None, "mp", None),
            P("mp", None),
            P(None, None, "mp"),
            P("mp", None),
        ),
        out_specs=(
            P(SEQ, "mp"),
            P(SEQ, "mp"),
            P(SEQ, "mp"),
            P(SEQ, "mp"),
            P(SEQ, "mp"),
            P(None, SEQ, None),
            P("mp", SEQ),
        ),
        check_vma=False,
    )
```

```python
from functools import partial

import jax
import jax.numpy as jnp
from jax import lax
from jax.experimental import pallas as pl
from jax.experimental.pallas import tpu as pltpu
from jax.sharding import Mesh
from jax.sharding import PartitionSpec as P

BLOCK = 128
SEQ = ("seq_0", "seq_1", "seq_2")
EPSILON = 1e-06
MP = 4
INTERPRET = False
F32 = jnp.float32
BF16 = jnp.bfloat16


PAD = 16


def exchange(value, axis):
    return lax.all_to_all(value, axis, split_axis=0, concat_axis=0, tiled=True)


def dot(left, right, dims):
    return lax.dot_general(left, right, (dims, ((), ())), preferred_element_type=F32)


NN = ((1,), (0,))
NT = ((1,), (1,))
TN = ((0,), (0,))


def facts_kernel(blocks_ref, fill_ref, plan_ref, out_ref):
    docs = blocks_ref.shape[1]
    counts = jnp.broadcast_to(blocks_ref[...], (PAD, docs)).astype(F32)
    fills = fill_ref[...].astype(F32)
    row = lax.broadcasted_iota(jnp.int32, (docs, docs), 0)
    col = lax.broadcasted_iota(jnp.int32, (docs, docs), 1)
    ends = dot(counts.astype(BF16), (row <= col).astype(BF16), NN)[:1]
    starts = ends - counts[:1]
    order = lax.broadcasted_iota(jnp.int32, (1, docs), 1).astype(F32)
    index = lax.broadcasted_iota(jnp.int32, plan_ref.shape, 1).astype(F32)
    owners = []
    for t in range(2):
        slot = 2 * lax.axis_index(SEQ) + t
        mine = jnp.sum(jnp.where(plan_ref[...] == slot, index, 0.0), axis=1, keepdims=True)
        inside = (starts <= mine) & (mine < ends)
        last = inside & (ends - 1.0 == mine)
        short = jnp.sum(jnp.where(last, BLOCK - fills, 0.0))
        out_ref[t] = BLOCK - short.astype(jnp.int32)
        owners.append(jnp.sum(jnp.where(inside, order, 0.0)).astype(jnp.int32))
    out_ref[2] = (owners[0] == owners[1]).astype(jnp.int32)
    out_ref[3] = lax.axis_index("mp")
    out_ref[4] = lax.axis_index("seq_2")


def call(kernel, out_shape, *args, scratch=(), smem=0, out=pltpu.VMEM, mib=16, name=None):
    spaces = [pltpu.SMEM] * smem + [pltpu.VMEM] * (len(args) - smem)
    one = not isinstance(out_shape, tuple)
    outs = [out] * (1 if one else len(out_shape))
    outs = [pl.BlockSpec(memory_space=o) for o in outs]
    return pl.pallas_call(
        kernel,
        in_specs=[pl.BlockSpec(memory_space=s) for s in spaces],
        out_specs=outs[0] if one else tuple(outs),
        out_shape=out_shape,
        scratch_shapes=scratch,
        interpret=INTERPRET,
        compiler_params=pltpu.CompilerParams(vmem_limit_bytes=mib * 2**20),
        name=name,
    )(*args)


def put(ref, at, values):
    for j in range(ref.shape[0]):
        ref[pl.ds(j, 1), at, :] = values[None, :, j * 128 : (j + 1) * 128]


def get(ref, at):
    return jnp.concatenate([ref[pl.ds(j, 1), at, :][0] for j in range(ref.shape[0])], axis=1)


def pack_kernel(streams_ref, out_ref, rows_ref):
    width = streams_ref.shape[0] // 4
    gap = jnp.zeros((out_ref.shape[1] - width, streams_ref.shape[1]), F32)
    for k in range(4):
        stream = streams_ref[k * width : (k + 1) * width, :].astype(F32)
        rows = jnp.concatenate([stream, gap], axis=0).T
        for t in range(2):
            at = pl.ds(4 * t + k, BLOCK, stride=8)
            put(rows_ref, at, rows[t * BLOCK : (t + 1) * BLOCK])
    out_ref[...] = get(rows_ref, slice(None)).astype(BF16)


def reorder_kernel(plan_ref, held_ref, keyval_ref, out_ref, *refs):
    *piece_refs, rows_ref, next_ref = refs
    for k, piece_ref in enumerate(piece_refs):
        piece_ref[...] = keyval_ref[((lax.axis_index("mp") + k) % MP) // 2]
    blocks = plan_ref.shape[1]
    slot = lax.broadcasted_iota(jnp.int32, (blocks, blocks), 0)
    pick = (plan_ref[...] == slot).astype(BF16)
    put(rows_ref, slice(None), held_ref[...].astype(F32))
    for k in range(4):
        at = pl.ds(k, blocks, stride=4)
        put(next_ref, at, dot(pick, get(rows_ref, at).astype(BF16), NN))
    out_ref[...] = get(next_ref, slice(None)).astype(BF16)


def unpack_kernel(rows_in_ref, send_ref, kept_ref, rows_ref):
    width = kept_ref.shape[0] // 4
    put(rows_ref, slice(None), rows_in_ref[...].astype(F32))
    for k in range(4):
        halves = [get(rows_ref, pl.ds(4 * t + k, BLOCK, stride=8)).T for t in range(2)]
        stream = jnp.concatenate(halves, axis=1)[:width].astype(BF16)
        at = slice(k * width, (k + 1) * width)
        kept_ref[at, :] = stream
        if k < 2:
            send_ref[at, :] = stream


def turn(value, by):
    return lax.ppermute(value, "mp", [(i, (i + by) % MP) for i in range(MP)])


def to_slots(streams, kv_weight, *tables):
    peers = lax.axis_size(SEQ)
    plan = tables[-1]
    share = BLOCK // peers
    width = streams[0].shape[0]
    lanes = -(-width // 128) * 128
    rows = 8 * BLOCK
    piece = jax.ShapeDtypeStruct(kv_weight.shape[1:], BF16)
    scratch = pltpu.VMEM((lanes // 128, rows, 128), F32)
    sent = call(
        pack_kernel,
        jax.ShapeDtypeStruct((rows, lanes), BF16),
        jnp.concatenate(streams, axis=0),
        scratch=[scratch],
        name="pack",
    )
    facts = call(
        facts_kernel,
        jax.ShapeDtypeStruct((5,), jnp.int32),
        *[table.reshape(1, -1) for table in tables],
        out=pltpu.SMEM,
        name="facts",
    )
    with jax.named_scope("hop_one"):
        held = exchange(sent.reshape(peers, share * 8, lanes), SEQ)
    held = held.reshape(peers, share, 8, lanes)
    placed = []
    for r in range(share):
        moved, *pieces = call(
            reorder_kernel,
            (jax.ShapeDtypeStruct((peers * 8, lanes), BF16), *[piece] * MP),
            plan.reshape(1, -1),
            held[:, r].reshape(peers * 8, lanes),
            kv_weight,
            scratch=[pltpu.VMEM((lanes // 128, peers * 8, 128), F32)] * 2,
            name="reorder",
        )
        placed.append(moved.reshape(peers, 8, lanes))
    placed = placed[0] if share == 1 else jnp.stack(placed, axis=1).reshape(peers, -1, lanes)
    with jax.named_scope("weights"):
        pieces = [pieces[0]] + [turn(pieces[k], k) for k in range(1, MP)]
    with jax.named_scope("hop_two"):
        owned = exchange(placed, SEQ)
    return facts, pieces, *call(
        unpack_kernel,
        (
            jax.ShapeDtypeStruct((2 * width, 2 * BLOCK), BF16),
            jax.ShapeDtypeStruct((4 * width, 2 * BLOCK), BF16),
        ),
        owned.reshape(rows, lanes),
        scratch=[scratch],
        name="unpack",
    )


def assemble(rows_ref, whole_ref, first):
    parts, both, _ = rows_ref.shape
    width = both // 2
    for m in range(parts):
        whole_ref[m * width : (m + 1) * width, :] = rows_ref[m, first : first + width, :]


def normalized(whole_ref):
    values = whole_ref[...].astype(F32)
    inverse = lax.rsqrt(jnp.mean(values * values, axis=0, keepdims=True) + EPSILON)
    return (values * inverse).astype(BF16), inverse


def row_sums(values, width):
    ones = jnp.ones((PAD, values.shape[1]), F32)
    sums = lax.dot_general(
        ones, values, (NT, ((), ())), preferred_element_type=F32, precision=lax.Precision.HIGHEST
    )
    return (sums / width).astype(BF16)


def feed_forward_kernel(
    rows_ref, gate_up_ref, down_ref, out_ref, inverse_ref, first_ref, second_ref
):
    parts, both, count = rows_ref.shape
    width = both // 2
    assemble(rows_ref, first_ref, 0)
    assemble(rows_ref, second_ref, width)
    normed, inverse_ref[...] = normalized(first_ref)
    normed = normed.T
    gate = dot(normed, gate_up_ref[0], NN)
    up = dot(normed, gate_up_ref[1], NN)
    dh = dot(second_ref[...].T, down_ref[...], NT)
    sigma = jax.nn.sigmoid(gate)
    silu = gate * sigma
    hidden = (silu * up).astype(BF16)
    d_gate = (dh * up * sigma * (1.0 + gate * (1.0 - sigma))).astype(BF16)
    d_up = (dh * silu).astype(BF16)
    inner = row_sums(d_gate.astype(F32) * gate + d_up.astype(F32) * up, parts * width)
    mixed = dot(hidden, down_ref[...], NN).astype(BF16).T
    for m in range(parts):
        at = slice(m * width, (m + 1) * width)
        out_ref[m, :width, :] = mixed[at]
        out_ref[m, width:both, :] = (
            dot(gate_up_ref[0, at, :], d_gate, NT) + dot(gate_up_ref[1, at, :], d_up, NT)
        ).astype(BF16)
        out_ref[m, both:, :] = inner


def live_columns(facts_ref, shape):
    column = lax.broadcasted_iota(jnp.int32, shape, 1)
    return column < jnp.where(column < BLOCK, facts_ref[0], facts_ref[1] + BLOCK)


def middle_kernel(
    facts_ref, parts_ref, kept_ref, inverse_ref, second_ref, first_cot_ref, send_ref
):
    parts, rows, count = parts_ref.shape
    width = (rows - PAD) // 2
    total = parts_ref[0].astype(F32)
    for m in range(1, parts):
        total += parts_ref[m].astype(F32)
    inverse = inverse_ref[...]
    first = kept_ref[:width, :].astype(F32)
    second = kept_ref[2 * width : 3 * width, :].astype(F32)
    cot = kept_ref[3 * width :, :].astype(F32)
    second = (second - total[:width]).astype(BF16)
    d_norm = total[width : 2 * width]
    inner = total[2 * width : 2 * width + 1]
    cot = (cot + (d_norm - first * inverse * inner) * inverse).astype(BF16)
    second_ref[...] = second
    first_cot_ref[...] = cot
    masked = jnp.where(live_columns(facts_ref, cot.shape), cot.astype(F32), 0.0).astype(BF16)
    send_ref[:width, :] = second
    send_ref[width:, :] = masked


def last_kernel(
    facts_ref, *refs
):
    *parts, kept_ref, second_ref, inverse_ref, first_ref, cot_ref = refs
    width = second_ref.shape[0]
    total = parts[0][...].astype(F32)
    for part in parts[1:]:
        total += part[...].astype(F32)
    attn = total[:width]
    d_norm = total[width : 2 * width]
    inner = total[2 * width : 2 * width + 1]
    inverse = inverse_ref[...]
    first = kept_ref[:width, :].astype(F32)
    cot = kept_ref[width : 2 * width, :].astype(F32)
    live = live_columns(facts_ref, attn.shape)
    first_ref[...] = (first - jnp.where(live, attn, 0.0)).astype(BF16)
    normed = second_ref[...].astype(F32) * inverse
    cot_ref[...] = (cot + (d_norm - normed * inner) * inverse).astype(BF16)


def attention_kernel(groups, facts_ref, rows_ref, query_ref, proj_ref, *refs):
    parts, both, count = rows_ref.shape
    width = both // 2
    pieces, refs = refs[:parts], refs[parts:]
    kept_ref, given_ref, makings_ref, keyval_ref, inner_ref, inverse_ref = refs[:6]
    second_ref, cot_ref, grads_ref = refs[6:]
    me = facts_ref[3]
    for k in range(parts):
        keyval_ref[(me + parts - k) % parts] = pieces[k][...]
    assemble(rows_ref, second_ref, 0)
    assemble(rows_ref, cot_ref, width)
    normed, inverse_ref[...] = normalized(second_ref)
    turned = normed.T
    whole = keyval_ref[...].reshape(parts * width, -1)
    query = dot(turned, query_ref[...].reshape(parts * width, -1), NN).astype(BF16)
    keyval = dot(turned, whole, NN).astype(BF16)
    d_out = dot(cot_ref[...].T, proj_ref[...], NT).astype(BF16)
    half = keyval.shape[1] // 2
    low = lax.broadcasted_iota(jnp.int32, keyval.shape, 1) < half
    wide = keyval.astype(F32)
    rolled = pltpu.roll(wide, half, 1)
    keys = jnp.where(low, wide, rolled).astype(BF16)
    values = jnp.where(low, rolled, wide).astype(BF16)
    row = lax.broadcasted_iota(jnp.int32, (count, count), 0)
    col = lax.broadcasted_iota(jnp.int32, (count, count), 1)
    together = (facts_ref[2] == 1) | ((row >= BLOCK) == (col >= BLOCK))
    allowed = (col <= row) & together & (live_columns(facts_ref, (count, count)) | (col == row))
    scale = 1.0 / (half**0.5)
    heads = d_query = d_key = d_value = 0.0
    for h in range(2):
        own = low if h == 0 else jnp.logical_not(low)
        zero = jnp.zeros_like(query)
        scores = dot(jnp.where(own, query, zero), keys, NT) * scale
        scores = jnp.where(allowed, scores, -1e30)
        expo = jnp.exp(scores - jnp.max(scores, axis=-1, keepdims=True))
        probs = expo / jnp.sum(expo, axis=-1, keepdims=True)
        probs_b = probs.astype(BF16)
        heads += jnp.where(own, dot(probs_b, values, NN), 0.0)
        d_prob = dot(jnp.where(own, d_out, zero), values, NT)
        delta = jnp.sum(probs * d_prob, axis=-1, keepdims=True)
        d_score = (probs * (d_prob - delta) * scale).astype(BF16)
        d_query += jnp.where(own, dot(d_score, keys, NN), 0.0)
        d_key += jnp.where(own, dot(d_score, query, TN), 0.0)
        d_value += jnp.where(own, dot(probs_b, d_out, TN), 0.0)
    heads = heads.astype(BF16)
    d_query = d_query.astype(BF16)
    d_key = d_key + pltpu.roll(d_key, half, 1)
    d_value = d_value + pltpu.roll(d_value, half, 1)
    d_keyval = jnp.where(low, d_key, d_value).astype(BF16)
    makings_ref[0] = heads
    makings_ref[1] = d_query
    makings_ref[2] = d_keyval
    inner_ref[...] = row_sums(
        d_query.astype(F32) * query.astype(F32) + d_keyval.astype(F32) * wide, parts * width
    )
    lines = 8 * width // 7
    spread = lax.broadcasted_iota(jnp.int32, (lines, width), 0)
    core = (spread >= lines // 2).astype(jnp.int32)
    place = (spread - core * (lines // 2)) // 8
    group = (2 * (place // groups) + core) * groups + place % groups
    source = jnp.where(spread % 8 < 7, 7 * group + spread % 8, -1)
    pick = (lax.broadcasted_iota(jnp.int32, source.shape, 1) == source).astype(BF16)
    for m in range(parts):
        at = slice(m * width, (m + 1) * width)
        grads = [dot(normed[at], d_query, NN), dot(normed[at], d_keyval, NN)]
        grads.append(dot(cot_ref[at, :], heads, NN))
        grads = jnp.concatenate(grads, axis=1).astype(BF16)
        grads = dot(pick, grads, NN).astype(BF16)
        to = slice(m * (lines // 2), (m + 1) * (lines // 2))
        for c in range(2):
            grads_ref[c, to, :] = grads[c * (lines // 2) : (c + 1) * (lines // 2)]
    kept_ref[...] = grads_ref[facts_ref[4]]
    given_ref[...] = grads_ref[1 - facts_ref[4]]


def pieces_kernel(
    facts_ref, makings_ref, keyval_ref, inner_ref, query_ref, proj_ref, *refs
):
    parts, width, _ = query_ref.shape
    both = 2 * width
    out_refs, turned_ref = refs[:parts], refs[parts]
    me = facts_ref[3]
    heads, d_query, d_keyval = makings_ref[0], makings_ref[1], makings_ref[2]
    turned_ref[...] = proj_ref[...].T.reshape(turned_ref.shape)
    for k in range(parts):
        m = (me + k) % parts
        out_refs[k][:width, :] = dot(turned_ref[m], heads, NT).astype(BF16)
        out_refs[k][width:both, :] = (
            dot(query_ref[m], d_query, NT) + dot(keyval_ref[m], d_keyval, NT)
        ).astype(BF16)
        out_refs[k][both:, :] = inner_ref[...]


def add_kernel(left_ref, right_ref, out_ref):
    out_ref[...] = (left_ref[...].astype(F32) + right_ref[...].astype(F32)).astype(BF16)


def finish_kernel(grads_ref, query_ref, out_ref, own_ref):
    total = jnp.sum(grads_ref[...].astype(F32), axis=0)
    total = total.reshape(-1, 8, total.shape[1])[:, :7].reshape(-1, total.shape[1])
    query_ref[...] = total[:, :128]
    out_ref[...] = total[:, 256:]
    for m in range(MP):
        own_ref[m] = total[:, 128:256]


def pair_kernel(shares_ref, out_ref):
    groups = out_ref.shape[1]
    per = MP // groups
    for g in range(groups):
        out_ref[:, g, :] = shares_ref[g * per] + shares_ref[g * per + 1]


def shards(
    y_first,
    y_second,
    grad_first,
    grad_second,
    doc_blocks,
    last_fill,
    plan,
    q_weight,
    kv_weight,
    out_weight,
    gate_up,
    down_weight,
):
    count, width = y_first.shape
    seq_size = lax.axis_size(SEQ)
    groups = kv_weight.shape[0]
    streams = (y_first.T, grad_second.T, y_second.T, grad_first.T)
    facts, pieces, send, kept = to_slots(streams, kv_weight, doc_blocks, last_fill, plan)
    send, facts, pieces = lax.optimization_barrier((send, facts, pieces))
    stream = jax.ShapeDtypeStruct((width, count), BF16)
    line = jax.ShapeDtypeStruct((1, count), F32)
    part = jax.ShapeDtypeStruct((2 * width + PAD, count), BF16)
    with jax.named_scope("gather_one"):
        rows = lax.all_gather(send, "mp", axis=0)
    whole = pltpu.VMEM((MP * width, count), BF16)
    parts, r_one = call(
        feed_forward_kernel,
        (jax.ShapeDtypeStruct((MP, *part.shape), BF16), line),
        rows,
        gate_up,
        down_weight,
        scratch=[whole, whole],
        name="feed_forward",
    )
    with jax.named_scope("sum_one"):
        parts = exchange(parts, "mp")
    second_in, first_cot, send = call(
        middle_kernel,
        (stream, stream, jax.ShapeDtypeStruct((2 * width, count), BF16)),
        facts,
        parts,
        kept,
        r_one,
        smem=1,
        name="middle",
    )
    with jax.named_scope("gather_two"):
        rows = lax.all_gather(send, "mp", axis=0)
    query = q_weight.reshape(MP, width, -1)
    half = jax.ShapeDtypeStruct((4 * BLOCK, 384), BF16)
    kept_grads, given, makings, keyval, inner, r_two = call(
        partial(attention_kernel, BLOCK // seq_size),
        (
            half,
            half,
            jax.ShapeDtypeStruct((3, count, 128), BF16),
            jax.ShapeDtypeStruct((MP, width, 128), BF16),
            jax.ShapeDtypeStruct((PAD, count), BF16),
            line,
        ),
        facts,
        rows,
        query,
        out_weight,
        *pieces,
        scratch=[whole, whole, pltpu.VMEM((2, *half.shape), BF16)],
        smem=1,
        name="attention",
    )
    with jax.named_scope("core_sum"):
        given = lax.ppermute(given, "seq_2", [(0, 1), (1, 0)])
    grads = call(add_kernel, half, kept_grads, given, name="add")
    with jax.named_scope("weight_grads"):
        grads = exchange(grads.reshape(seq_size // 2, -1, grads.shape[1]), SEQ[:2])
    parts = call(
        pieces_kernel,
        (part,) * MP,
        facts,
        makings,
        keyval,
        inner,
        query,
        out_weight,
        scratch=[pltpu.VMEM((MP, width, 128), BF16)],
        smem=1,
        name="pieces",
    )
    with jax.named_scope("last_sum"):
        parts = [parts[0]] + [turn(parts[k], k) for k in range(1, MP)]
    first_in, second_cot = call(
        last_kernel, (stream, stream), facts, *parts, kept, second_in, r_two, smem=1, name="last"
    )
    share = jax.ShapeDtypeStruct((7 * BLOCK // seq_size, 128), F32)
    query_grad, out_grad, own = call(
        finish_kernel,
        (share, share, jax.ShapeDtypeStruct((MP, *share.shape), F32)),
        grads,
        name="finish",
    )
    with jax.named_scope("key_grads"):
        shares = exchange(own, "mp")
    kv_grad = call(
        pair_kernel,
        jax.ShapeDtypeStruct((shares.shape[1], groups, 128), F32),
        shares,
        name="pair",
    )
    return (
        first_in.T,
        second_in.T,
        first_cot.T,
        second_cot.T,
        query_grad,
        kv_grad.transpose(1, 0, 2),
        out_grad.T,
    )


def solution(mesh):
    if "seq" in mesh.shape and mesh.shape["seq"] == 128:
        shape = (8, 8, 2, MP)
    else:
        shape = (2, 2, 2, MP)
    finer = Mesh(mesh.devices.reshape(shape), ("seq_0", "seq_1", "seq_2", "mp"))
    return jax.shard_map(
        shards,
        mesh=finer,
        in_specs=(
            P(SEQ, "mp"),
            P(SEQ, "mp"),
            P(SEQ, "mp"),
            P(SEQ, "mp"),
            P(),
            P(),
            P(),
            P(None, "mp"),
            P(None, "mp", None),
            P("mp", None),
            P(None, None, "mp"),
            P("mp", None),
        ),
        out_specs=(
            P(SEQ, "mp"),
            P(SEQ, "mp"),
            P(SEQ, "mp"),
            P(SEQ, "mp"),
            P(SEQ, "mp"),
            P(None, SEQ, None),
            P("mp", SEQ),
        ),
        check_vma=False,
    )
```

```python
from functools import partial

import jax
import jax.numpy as jnp
from jax import lax
from jax.experimental import pallas as pl
from jax.experimental.pallas import tpu as pltpu
from jax.sharding import Mesh
from jax.sharding import PartitionSpec as P

BLOCK = 128
SEQ = ("seq_0", "seq_1", "seq_2")
EPSILON = 1e-06
MP = 4
INTERPRET = False
F32 = jnp.float32
BF16 = jnp.bfloat16


PAD = 16


def exchange(value, axis):
    return lax.all_to_all(value, axis, split_axis=0, concat_axis=0, tiled=True)


def dot(left, right, dims):
    return lax.dot_general(left, right, (dims, ((), ())), preferred_element_type=F32)


NN = ((1,), (0,))
NT = ((1,), (1,))
TN = ((0,), (0,))


def facts_kernel(blocks_ref, fill_ref, plan_ref, out_ref):
    docs = blocks_ref.shape[1]
    counts = jnp.broadcast_to(blocks_ref[...], (PAD, docs)).astype(F32)
    fills = fill_ref[...].astype(F32)
    row = lax.broadcasted_iota(jnp.int32, (docs, docs), 0)
    col = lax.broadcasted_iota(jnp.int32, (docs, docs), 1)
    ends = dot(counts.astype(BF16), (row <= col).astype(BF16), NN)[:1]
    starts = ends - counts[:1]
    order = lax.broadcasted_iota(jnp.int32, (1, docs), 1).astype(F32)
    index = lax.broadcasted_iota(jnp.int32, plan_ref.shape, 1).astype(F32)
    owners = []
    for t in range(2):
        slot = 2 * lax.axis_index(SEQ) + t
        mine = jnp.sum(jnp.where(plan_ref[...] == slot, index, 0.0), axis=1, keepdims=True)
        inside = (starts <= mine) & (mine < ends)
        last = inside & (ends - 1.0 == mine)
        short = jnp.sum(jnp.where(last, BLOCK - fills, 0.0))
        out_ref[t] = BLOCK - short.astype(jnp.int32)
        owners.append(jnp.sum(jnp.where(inside, order, 0.0)).astype(jnp.int32))
    out_ref[2] = (owners[0] == owners[1]).astype(jnp.int32)
    out_ref[3] = lax.axis_index("mp")
    out_ref[4] = lax.axis_index("seq_2")


def call(kernel, out_shape, *args, scratch=(), smem=0, out=pltpu.VMEM, mib=16):
    spaces = [pltpu.SMEM] * smem + [pltpu.VMEM] * (len(args) - smem)
    one = not isinstance(out_shape, tuple)
    outs = [out] * (1 if one else len(out_shape))
    outs = [pl.BlockSpec(memory_space=o) for o in outs]
    return pl.pallas_call(
        kernel,
        in_specs=[pl.BlockSpec(memory_space=s) for s in spaces],
        out_specs=outs[0] if one else tuple(outs),
        out_shape=out_shape,
        scratch_shapes=scratch,
        interpret=INTERPRET,
        compiler_params=pltpu.CompilerParams(vmem_limit_bytes=mib * 2**20),
    )(*args)


def put(ref, at, values):
    for j in range(ref.shape[0]):
        ref[pl.ds(j, 1), at, :] = values[None, :, j * 128 : (j + 1) * 128]


def get(ref, at):
    return jnp.concatenate([ref[pl.ds(j, 1), at, :][0] for j in range(ref.shape[0])], axis=1)


def pack_kernel(streams_ref, keyval_ref, out_ref, *refs):
    *piece_refs, rows_ref = refs
    for k, piece_ref in enumerate(piece_refs):
        piece_ref[...] = keyval_ref[((lax.axis_index("mp") + k) % MP) // 2]
    width = streams_ref.shape[0] // 4
    gap = jnp.zeros((out_ref.shape[1] - width, streams_ref.shape[1]), F32)
    for k in range(4):
        stream = streams_ref[k * width : (k + 1) * width, :].astype(F32)
        rows = jnp.concatenate([stream, gap], axis=0).T
        for t in range(2):
            at = pl.ds(4 * t + k, BLOCK, stride=8)
            put(rows_ref, at, rows[t * BLOCK : (t + 1) * BLOCK])
    out_ref[...] = get(rows_ref, slice(None)).astype(BF16)


def reorder_kernel(plan_ref, held_ref, *refs):
    *out_refs, rows_ref, next_ref = refs
    blocks = plan_ref.shape[1]
    slot = lax.broadcasted_iota(jnp.int32, (blocks, blocks), 0)
    pick = (plan_ref[...] == slot).astype(BF16)
    put(rows_ref, slice(None), held_ref[...].astype(F32))
    for k in range(4):
        rows = dot(pick, get(rows_ref, pl.ds(k, blocks, stride=4)).astype(BF16), NN)
        for j in range(2):
            at = pl.ds(2 * (k % 2) + j, blocks, stride=4)
            next_ref[pl.ds(k // 2, 1), at, :] = rows[None, :, j * 128 : (j + 1) * 128]
    for h, out_ref in enumerate(out_refs):
        out_ref[...] = next_ref[h].astype(BF16)


def unpack_kernel(rows_in_ref, *refs):
    *out_refs, rows_ref = refs
    width = out_refs[0].shape[0] // 2
    rows_ref[0] = rows_in_ref[...].astype(F32)
    for k in range(2):
        halves = []
        for t in range(2):
            lanes = [
                rows_ref[pl.ds(0, 1), pl.ds(4 * t + 2 * k + j, BLOCK, stride=8), :][0].T
                for j in range(2)
            ]
            halves.append(jnp.concatenate(lanes, axis=0)[:width])
        stream = jnp.concatenate(halves, axis=1).astype(BF16)
        for out_ref in out_refs:
            out_ref[k * width : (k + 1) * width, :] = stream


def unpack(owned, width, copies):
    rows = 8 * BLOCK
    return call(
        unpack_kernel,
        (jax.ShapeDtypeStruct((2 * width, 2 * BLOCK), BF16),) * copies,
        owned.reshape(rows, 128),
        scratch=[pltpu.VMEM((1, rows, 128), F32)],
    )


def turn(value, by):
    return lax.ppermute(value, "mp", [(i, (i + by) % MP) for i in range(MP)])


def to_slots(streams, kv_weight, *tables):
    peers = lax.axis_size(SEQ)
    plan = tables[-1]
    share = BLOCK // peers
    width = streams[0].shape[0]
    lanes = -(-width // 128) * 128
    rows = 8 * BLOCK
    piece = jax.ShapeDtypeStruct(kv_weight.shape[1:], BF16)
    scratch = pltpu.VMEM((lanes // 128, rows, 128), F32)
    sent, *pieces = call(
        pack_kernel,
        (jax.ShapeDtypeStruct((rows, lanes), BF16), *[piece] * MP),
        jnp.concatenate(streams, axis=0),
        kv_weight,
        scratch=[scratch],
    )
    facts = call(
        facts_kernel,
        jax.ShapeDtypeStruct((5,), jnp.int32),
        *[table.reshape(1, -1) for table in tables],
        out=pltpu.SMEM,
    )
    held = exchange(sent.reshape(peers, share * 8, lanes), SEQ)
    pieces = [pieces[0]] + [turn(pieces[k], k) for k in range(1, MP)]
    held = held.reshape(peers, share, 8, lanes)
    placed = []
    for r in range(share):
        placed.append(
            call(
                reorder_kernel,
                (jax.ShapeDtypeStruct((peers * 8, 128), BF16),) * 2,
                plan.reshape(1, -1),
                held[:, r].reshape(peers * 8, lanes),
                scratch=[pltpu.VMEM((2, peers * 8, 128), F32)] * 2,
            )
        )
    owned = []
    for h in range(2):
        halves = [p[h].reshape(peers, 8, 128) for p in placed]
        halves = halves[0] if share == 1 else jnp.stack(halves, axis=1).reshape(peers, -1, 128)
        owned.extend(unpack(exchange(halves, SEQ), width, 3 - 2 * h))
    return facts, pieces, *owned


def around(value):
    return [value] + [turn(value, k) for k in range(1, MP)]


def assemble(me, pieces, whole_ref, first):
    parts, width, _ = whole_ref.shape
    for k, piece in enumerate(pieces):
        whole_ref[(me + parts - k) % parts] = piece[first : first + width, :]


def normalized(whole_ref):
    values = merged(whole_ref).astype(F32)
    inverse = lax.rsqrt(jnp.mean(values * values, axis=0, keepdims=True) + EPSILON)
    return (values * inverse).astype(BF16), inverse


def merged(ref):
    values = ref[...]
    return values.reshape(-1, values.shape[-1])


def row_sums(values, width):
    ones = jnp.ones((PAD, values.shape[1]), F32)
    sums = lax.dot_general(
        ones, values, (NT, ((), ())), preferred_element_type=F32, precision=lax.Precision.HIGHEST
    )
    return (sums / width).astype(BF16)


def feed_forward_kernel(facts_ref, *refs):
    pieces, refs = refs[:MP], refs[MP:]
    gate_up_ref, down_ref = refs[:2]
    out_refs = refs[2 : 2 + MP]
    inverse_ref, first_ref, second_ref, mixed_ref = refs[2 + MP :]
    gate_ref, up_ref = gate_up_ref.at[0], gate_up_ref.at[1]
    parts, width, _ = first_ref.shape
    both = 2 * width
    me = facts_ref[3]
    assemble(me, pieces, first_ref, 0)
    assemble(me, pieces, second_ref, width)
    normed, inverse_ref[...] = normalized(first_ref)
    normed = normed.T
    gate = dot(normed, merged(gate_ref), NN)
    up = dot(normed, merged(up_ref), NN)
    dh = dot(merged(second_ref).T, down_ref[...], NT)
    sigma = jax.nn.sigmoid(gate)
    silu = gate * sigma
    hidden = (silu * up).astype(BF16)
    d_gate = (dh * up * sigma * (1.0 + gate * (1.0 - sigma))).astype(BF16)
    d_up = (dh * silu).astype(BF16)
    inner = row_sums(d_gate.astype(F32) * gate + d_up.astype(F32) * up, parts * width)
    mixed_ref[...] = dot(hidden, down_ref[...], NN).astype(BF16).T.reshape(mixed_ref.shape)
    for k in range(parts):
        m = (me + k) % parts
        out_refs[k][:width, :] = mixed_ref[m]
        out_refs[k][width:both, :] = (
            dot(gate_ref[m], d_gate, NT) + dot(up_ref[m], d_up, NT)
        ).astype(BF16)
        out_refs[k][both:, :] = inner


def live_columns(facts_ref, shape):
    column = lax.broadcasted_iota(jnp.int32, shape, 1)
    return column < jnp.where(column < BLOCK, facts_ref[0], facts_ref[1] + BLOCK)


def middle_kernel(facts_ref, *refs):
    parts, refs = refs[:MP], refs[MP:]
    first_half_ref, second_half_ref, inverse_ref, second_ref, first_cot_ref, send_ref = refs
    width = second_ref.shape[0]
    total = parts[0][...].astype(F32)
    for part in parts[1:]:
        total += part[...].astype(F32)
    inverse = inverse_ref[...]
    first = first_half_ref[:width, :].astype(F32)
    second = second_half_ref[:width, :].astype(F32)
    cot = second_half_ref[width:, :].astype(F32)
    second = (second - total[:width]).astype(BF16)
    d_norm = total[width : 2 * width]
    inner = total[2 * width : 2 * width + 1]
    cot = (cot + (d_norm - first * inverse * inner) * inverse).astype(BF16)
    second_ref[...] = second
    first_cot_ref[...] = cot
    masked = jnp.where(live_columns(facts_ref, cot.shape), cot.astype(F32), 0.0).astype(BF16)
    send_ref[:width, :] = second
    send_ref[width:, :] = masked


def last_kernel(
    facts_ref, *refs
):
    *parts, kept_ref, second_ref, inverse_ref, first_ref, cot_ref = refs
    width = second_ref.shape[0]
    total = parts[0][...].astype(F32)
    for part in parts[1:]:
        total += part[...].astype(F32)
    attn = total[:width]
    d_norm = total[width : 2 * width]
    inner = total[2 * width : 2 * width + 1]
    inverse = inverse_ref[...]
    first = kept_ref[:width, :].astype(F32)
    cot = kept_ref[width : 2 * width, :].astype(F32)
    live = live_columns(facts_ref, attn.shape)
    first_ref[...] = (first - jnp.where(live, attn, 0.0)).astype(BF16)
    normed = second_ref[...].astype(F32) * inverse
    cot_ref[...] = (cot + (d_norm - normed * inner) * inverse).astype(BF16)


def attention_kernel(groups, facts_ref, rows_ref, query_ref, proj_ref, *refs):
    parts, both, count = rows_ref.shape
    width = both // 2
    pieces, refs = refs[:parts], refs[parts:]
    kept_ref, given_ref, makings_ref, keyval_ref, inner_ref, inverse_ref = refs[:6]
    second_ref, cot_ref, grads_ref = refs[6:]
    me = facts_ref[3]
    for k in range(parts):
        keyval_ref[(me + parts - k) % parts] = pieces[k][...]
    for m in range(parts):
        second_ref[m] = rows_ref[m, :width, :]
        cot_ref[m] = rows_ref[m, width:, :]
    normed, inverse_ref[...] = normalized(second_ref)
    turned = normed.T
    whole = keyval_ref[...].reshape(parts * width, -1)
    query = dot(turned, query_ref[...].reshape(parts * width, -1), NN).astype(BF16)
    keyval = dot(turned, whole, NN).astype(BF16)
    d_out = dot(merged(cot_ref).T, proj_ref[...], NT).astype(BF16)
    half = keyval.shape[1] // 2
    low = lax.broadcasted_iota(jnp.int32, keyval.shape, 1) < half
    wide = keyval.astype(F32)
    rolled = pltpu.roll(wide, half, 1)
    keys = jnp.where(low, wide, rolled).astype(BF16)
    values = jnp.where(low, rolled, wide).astype(BF16)
    row = lax.broadcasted_iota(jnp.int32, (count, count), 0)
    col = lax.broadcasted_iota(jnp.int32, (count, count), 1)
    together = (facts_ref[2] == 1) | ((row >= BLOCK) == (col >= BLOCK))
    allowed = (col <= row) & together & (live_columns(facts_ref, (count, count)) | (col == row))
    scale = 1.0 / (half**0.5)
    heads = d_query = d_key = d_value = 0.0
    for h in range(2):
        own = low if h == 0 else jnp.logical_not(low)
        zero = jnp.zeros_like(query)
        scores = dot(jnp.where(own, query, zero), keys, NT) * scale
        scores = jnp.where(allowed, scores, -1e30)
        expo = jnp.exp(scores - jnp.max(scores, axis=-1, keepdims=True))
        probs = expo / jnp.sum(expo, axis=-1, keepdims=True)
        probs_b = probs.astype(BF16)
        heads += jnp.where(own, dot(probs_b, values, NN), 0.0)
        d_prob = dot(jnp.where(own, d_out, zero), values, NT)
        delta = jnp.sum(probs * d_prob, axis=-1, keepdims=True)
        d_score = (probs * (d_prob - delta) * scale).astype(BF16)
        d_query += jnp.where(own, dot(d_score, keys, NN), 0.0)
        d_key += jnp.where(own, dot(d_score, query, TN), 0.0)
        d_value += jnp.where(own, dot(probs_b, d_out, TN), 0.0)
    heads = heads.astype(BF16)
    d_query = d_query.astype(BF16)
    d_key = d_key + pltpu.roll(d_key, half, 1)
    d_value = d_value + pltpu.roll(d_value, half, 1)
    d_keyval = jnp.where(low, d_key, d_value).astype(BF16)
    makings_ref[0] = heads
    makings_ref[1] = d_query
    makings_ref[2] = d_keyval
    inner_ref[...] = row_sums(
        d_query.astype(F32) * query.astype(F32) + d_keyval.astype(F32) * wide, parts * width
    )
    lines = 8 * width // 7
    spread = lax.broadcasted_iota(jnp.int32, (lines, width), 0)
    core = (spread >= lines // 2).astype(jnp.int32)
    place = (spread - core * (lines // 2)) // 8
    group = (2 * (place // groups) + core) * groups + place % groups
    source = jnp.where(spread % 8 < 7, 7 * group + spread % 8, -1)
    pick = (lax.broadcasted_iota(jnp.int32, source.shape, 1) == source).astype(BF16)
    for m in range(parts):
        at = slice(m * width, (m + 1) * width)
        grads = [dot(normed[at], d_query, NN), dot(normed[at], d_keyval, NN)]
        grads.append(dot(cot_ref[m], heads, NN))
        grads = jnp.concatenate(grads, axis=1).astype(BF16)
        grads = dot(pick, grads, NN).astype(BF16)
        to = slice(m * (lines // 2), (m + 1) * (lines // 2))
        for c in range(2):
            grads_ref[c, to, :] = grads[c * (lines // 2) : (c + 1) * (lines // 2)]
    kept_ref[...] = grads_ref[facts_ref[4]]
    given_ref[...] = grads_ref[1 - facts_ref[4]]


def pieces_kernel(
    facts_ref, makings_ref, keyval_ref, inner_ref, query_ref, proj_ref, *refs
):
    parts, width, _ = query_ref.shape
    both = 2 * width
    out_refs, turned_ref = refs[:parts], refs[parts]
    me = facts_ref[3]
    heads, d_query, d_keyval = makings_ref[0], makings_ref[1], makings_ref[2]
    turned_ref[...] = proj_ref[...].T.reshape(turned_ref.shape)
    for k in range(parts):
        m = (me + k) % parts
        out_refs[k][:width, :] = dot(turned_ref[m], heads, NT).astype(BF16)
        out_refs[k][width:both, :] = (
            dot(query_ref[m], d_query, NT) + dot(keyval_ref[m], d_keyval, NT)
        ).astype(BF16)
        out_refs[k][both:, :] = inner_ref[...]


def add_kernel(left_ref, right_ref, out_ref):
    out_ref[...] = (left_ref[...].astype(F32) + right_ref[...].astype(F32)).astype(BF16)


def finish_kernel(grads_ref, query_ref, out_ref, own_ref):
    total = jnp.sum(grads_ref[...].astype(F32), axis=0)
    total = total.reshape(-1, 8, total.shape[1])[:, :7].reshape(-1, total.shape[1])
    query_ref[...] = total[:, :128]
    out_ref[...] = total[:, 256:]
    for m in range(MP):
        own_ref[m] = total[:, 128:256]


def pair_kernel(shares_ref, out_ref):
    groups = out_ref.shape[1]
    per = MP // groups
    for g in range(groups):
        out_ref[:, g, :] = shares_ref[g * per] + shares_ref[g * per + 1]


def shards(
    y_first,
    y_second,
    grad_first,
    grad_second,
    doc_blocks,
    last_fill,
    plan,
    q_weight,
    kv_weight,
    out_weight,
    gate_up,
    down_weight,
):
    count, width = y_first.shape
    seq_size = lax.axis_size(SEQ)
    groups = kv_weight.shape[0]
    streams = (y_first.T, grad_second.T, y_second.T, grad_first.T)
    facts, pieces, send, near, kept, other = to_slots(streams, kv_weight, doc_blocks, last_fill, plan)
    stream = jax.ShapeDtypeStruct((width, count), BF16)
    line = jax.ShapeDtypeStruct((1, count), F32)
    part = jax.ShapeDtypeStruct((2 * width + PAD, count), BF16)
    whole = pltpu.VMEM((MP, width, count), BF16)
    rows = [near] + around(send)[1:]
    *parts, r_one = call(
        feed_forward_kernel,
        (*[part] * MP, line),
        facts,
        *rows,
        gate_up.reshape(2, MP, width, -1),
        down_weight,
        scratch=[whole] * 3,
        smem=1,
    )
    parts = [parts[0]] + [turn(parts[k], k) for k in range(1, MP)]
    second_in, first_cot, send = call(
        middle_kernel,
        (stream, stream, jax.ShapeDtypeStruct((2 * width, count), BF16)),
        facts,
        *parts,
        kept,
        other,
        r_one,
        smem=1,
    )
    rows = lax.all_gather(send, "mp", axis=0)
    query = q_weight.reshape(MP, width, -1)
    half = jax.ShapeDtypeStruct((4 * BLOCK, 384), BF16)
    kept_grads, given, makings, keyval, inner, r_two = call(
        partial(attention_kernel, BLOCK // seq_size),
        (
            half,
            half,
            jax.ShapeDtypeStruct((3, count, 128), BF16),
            jax.ShapeDtypeStruct((MP, width, 128), BF16),
            jax.ShapeDtypeStruct((PAD, count), BF16),
            line,
        ),
        facts,
        rows,
        query,
        out_weight,
        *pieces,
        scratch=[whole, whole, pltpu.VMEM((2, *half.shape), BF16)],
        smem=1,
    )
    given = lax.ppermute(given, "seq_2", [(0, 1), (1, 0)])
    grads = call(add_kernel, half, kept_grads, given)
    grads = exchange(grads.reshape(seq_size // 2, -1, grads.shape[1]), SEQ[:2])
    parts = call(
        pieces_kernel,
        (part,) * MP,
        facts,
        makings,
        keyval,
        inner,
        query,
        out_weight,
        scratch=[pltpu.VMEM((MP, width, 128), BF16)],
        smem=1,
    )
    parts = [parts[0]] + [turn(parts[k], k) for k in range(1, MP)]
    first_in, second_cot = call(
        last_kernel, (stream, stream), facts, *parts, kept, second_in, r_two, smem=1
    )
    share = jax.ShapeDtypeStruct((7 * BLOCK // seq_size, 128), F32)
    query_grad, out_grad, own = call(
        finish_kernel, (share, share, jax.ShapeDtypeStruct((MP, *share.shape), F32)), grads
    )
    shares = exchange(own, "mp")
    kv_grad = call(pair_kernel, jax.ShapeDtypeStruct((shares.shape[1], groups, 128), F32), shares)
    return (
        first_in.T,
        second_in.T,
        first_cot.T,
        second_cot.T,
        query_grad,
        kv_grad.transpose(1, 0, 2),
        out_grad.T,
    )


def solution(mesh):
    if "seq" in mesh.shape and mesh.shape["seq"] == 128:
        shape = (8, 8, 2, MP)
    else:
        shape = (2, 2, 2, MP)
    finer = Mesh(mesh.devices.reshape(shape), ("seq_0", "seq_1", "seq_2", "mp"))
    return jax.shard_map(
        shards,
        mesh=finer,
        in_specs=(
            P(SEQ, "mp"),
            P(SEQ, "mp"),
            P(SEQ, "mp"),
            P(SEQ, "mp"),
            P(),
            P(),
            P(),
            P(None, "mp"),
            P(None, "mp", None),
            P("mp", None),
            P(None, None, "mp"),
            P("mp", None),
        ),
        out_specs=(
            P(SEQ, "mp"),
            P(SEQ, "mp"),
            P(SEQ, "mp"),
            P(SEQ, "mp"),
            P(SEQ, "mp"),
            P(None, SEQ, None),
            P("mp", SEQ),
        ),
        check_vma=False,
    )
```

```python
from functools import partial

import jax
import jax.numpy as jnp
from jax import lax
from jax.experimental import pallas as pl
from jax.experimental.pallas import tpu as pltpu
from jax.sharding import Mesh
from jax.sharding import PartitionSpec as P

BLOCK = 128
SEQ = ("seq_0", "seq_1", "seq_2")
EPSILON = 1e-06
MP = 4
INTERPRET = False
F32 = jnp.float32
BF16 = jnp.bfloat16


PAD = 8


def exchange(value, axis):
    return lax.all_to_all(value, axis, split_axis=0, concat_axis=0, tiled=True)


def dot(left, right, dims):
    return lax.dot_general(left, right, (dims, ((), ())), preferred_element_type=F32)


NN = ((1,), (0,))
NT = ((1,), (1,))
TN = ((0,), (0,))


def facts_kernel(blocks_ref, fill_ref, plan_ref, out_ref):
    docs = blocks_ref.shape[1]
    counts = jnp.broadcast_to(blocks_ref[...], (8, docs)).astype(F32)
    fills = fill_ref[...].astype(F32)
    row = lax.broadcasted_iota(jnp.int32, (docs, docs), 0)
    col = lax.broadcasted_iota(jnp.int32, (docs, docs), 1)
    ends = dot(counts.astype(BF16), (row <= col).astype(BF16), NN)[:1]
    starts = ends - counts[:1]
    order = lax.broadcasted_iota(jnp.int32, (1, docs), 1).astype(F32)
    index = lax.broadcasted_iota(jnp.int32, plan_ref.shape, 1).astype(F32)
    owners = []
    for t in range(2):
        slot = 2 * lax.axis_index(SEQ) + t
        mine = jnp.sum(jnp.where(plan_ref[...] == slot, index, 0.0), axis=1, keepdims=True)
        inside = (starts <= mine) & (mine < ends)
        last = inside & (ends - 1.0 == mine)
        short = jnp.sum(jnp.where(last, BLOCK - fills, 0.0))
        out_ref[t] = BLOCK - short.astype(jnp.int32)
        owners.append(jnp.sum(jnp.where(inside, order, 0.0)).astype(jnp.int32))
    out_ref[2] = (owners[0] == owners[1]).astype(jnp.int32)
    out_ref[3] = lax.axis_index("mp")
    out_ref[4] = lax.axis_index("seq_2")


def call(kernel, out_shape, *args, scratch=(), smem=0, out=pltpu.VMEM, mib=16, name=None):
    spaces = [pltpu.SMEM] * smem + [pltpu.VMEM] * (len(args) - smem)
    one = not isinstance(out_shape, tuple)
    outs = [out] * (1 if one else len(out_shape))
    outs = [pl.BlockSpec(memory_space=o) for o in outs]
    return pl.pallas_call(
        kernel,
        in_specs=[pl.BlockSpec(memory_space=s) for s in spaces],
        out_specs=outs[0] if one else tuple(outs),
        out_shape=out_shape,
        scratch_shapes=scratch,
        interpret=INTERPRET,
        compiler_params=pltpu.CompilerParams(vmem_limit_bytes=mib * 2**20),
        name=name,
    )(*args)


def put(ref, at, values):
    for j in range(ref.shape[0]):
        ref[pl.ds(j, 1), at, :] = values[None, :, j * 128 : (j + 1) * 128]


def get(ref, at):
    return jnp.concatenate([ref[pl.ds(j, 1), at, :][0] for j in range(ref.shape[0])], axis=1)


def pack_kernel(streams_ref, out_ref, rows_ref):
    width = streams_ref.shape[0] // 4
    gap = jnp.zeros((out_ref.shape[1] - width, streams_ref.shape[1]), F32)
    for k in range(4):
        stream = streams_ref[k * width : (k + 1) * width, :].astype(F32)
        rows = jnp.concatenate([stream, gap], axis=0).T
        for t in range(2):
            at = pl.ds(4 * t + k, BLOCK, stride=8)
            put(rows_ref, at, rows[t * BLOCK : (t + 1) * BLOCK])
    out_ref[...] = get(rows_ref, slice(None)).astype(BF16)


def reorder_kernel(plan_ref, held_ref, keyval_ref, out_ref, *refs):
    *piece_refs, rows_ref, next_ref = refs
    for k, piece_ref in enumerate(piece_refs):
        piece_ref[...] = keyval_ref[((lax.axis_index("mp") + k) % MP) // 2]
    blocks = plan_ref.shape[1]
    slot = lax.broadcasted_iota(jnp.int32, (blocks, blocks), 0)
    pick = (plan_ref[...] == slot).astype(BF16)
    put(rows_ref, slice(None), held_ref[...].astype(F32))
    for k in range(4):
        at = pl.ds(k, blocks, stride=4)
        put(next_ref, at, dot(pick, get(rows_ref, at).astype(BF16), NN))
    out_ref[...] = get(next_ref, slice(None)).astype(BF16)


def unpack_kernel(rows_in_ref, send_ref, kept_ref, rows_ref):
    width = kept_ref.shape[0] // 4
    put(rows_ref, slice(None), rows_in_ref[...].astype(F32))
    for k in range(4):
        halves = [get(rows_ref, pl.ds(4 * t + k, BLOCK, stride=8)).T for t in range(2)]
        stream = jnp.concatenate(halves, axis=1)[:width].astype(BF16)
        at = slice(k * width, (k + 1) * width)
        kept_ref[at, :] = stream
        if k < 2:
            send_ref[at, :] = stream


def turn(value, by):
    return lax.ppermute(value, "mp", [(i, (i + by) % MP) for i in range(MP)])


def to_slots(streams, kv_weight, *tables):
    peers = lax.axis_size(SEQ)
    plan = tables[-1]
    share = BLOCK // peers
    width = streams[0].shape[0]
    lanes = -(-width // 128) * 128
    rows = 8 * BLOCK
    piece = jax.ShapeDtypeStruct(kv_weight.shape[1:], BF16)
    scratch = pltpu.VMEM((lanes // 128, rows, 128), F32)
    sent = call(
        pack_kernel,
        jax.ShapeDtypeStruct((rows, lanes), BF16),
        jnp.concatenate(streams, axis=0),
        scratch=[scratch],
        name="pack",
    )
    facts = call(
        facts_kernel,
        jax.ShapeDtypeStruct((5,), jnp.int32),
        *[table.reshape(1, -1) for table in tables],
        out=pltpu.SMEM,
        name="facts",
    )
    with jax.named_scope("hop_one"):
        held = exchange(sent.reshape(peers, share * 8, lanes), SEQ)
    held = held.reshape(peers, share, 8, lanes)
    placed = []
    for r in range(share):
        moved, *pieces = call(
            reorder_kernel,
            (jax.ShapeDtypeStruct((peers * 8, lanes), BF16), *[piece] * MP),
            plan.reshape(1, -1),
            held[:, r].reshape(peers * 8, lanes),
            kv_weight,
            scratch=[pltpu.VMEM((lanes // 128, peers * 8, 128), F32)] * 2,
            name="reorder",
        )
        placed.append(moved.reshape(peers, 8, lanes))
    placed = placed[0] if share == 1 else jnp.stack(placed, axis=1).reshape(peers, -1, lanes)
    with jax.named_scope("weights"):
        pieces = [pieces[0]] + [turn(pieces[k], k) for k in range(1, MP)]
    with jax.named_scope("hop_two"):
        owned = exchange(placed, SEQ)
    return facts, pieces, *call(
        unpack_kernel,
        (
            jax.ShapeDtypeStruct((2 * width, 2 * BLOCK), BF16),
            jax.ShapeDtypeStruct((4 * width, 2 * BLOCK), BF16),
        ),
        owned.reshape(rows, lanes),
        scratch=[scratch],
        name="unpack",
    )


def assemble(rows_ref, whole_ref, first):
    parts, both, _ = rows_ref.shape
    width = both // 2
    for m in range(parts):
        whole_ref[m * width : (m + 1) * width, :] = rows_ref[m, first : first + width, :]


def normalized(whole_ref):
    values = whole_ref[...].astype(F32)
    inverse = lax.rsqrt(jnp.mean(values * values, axis=0, keepdims=True) + EPSILON)
    return (values * inverse).astype(BF16), inverse


def row_sums(values, width):
    ones = jnp.ones((PAD, values.shape[1]), F32)
    sums = lax.dot_general(
        ones, values, (NT, ((), ())), preferred_element_type=F32, precision=lax.Precision.HIGHEST
    )
    return (sums / width).astype(BF16)


def feed_forward_kernel(
    rows_ref, gate_up_ref, down_ref, out_ref, inverse_ref, first_ref, second_ref
):
    parts, both, count = rows_ref.shape
    width = both // 2
    assemble(rows_ref, first_ref, 0)
    assemble(rows_ref, second_ref, width)
    normed, inverse_ref[...] = normalized(first_ref)
    normed = normed.T
    gate = dot(normed, gate_up_ref[0], NN)
    up = dot(normed, gate_up_ref[1], NN)
    dh = dot(second_ref[...].T, down_ref[...], NT)
    sigma = jax.nn.sigmoid(gate)
    silu = gate * sigma
    hidden = (silu * up).astype(BF16)
    d_gate = (dh * up * sigma * (1.0 + gate * (1.0 - sigma))).astype(BF16)
    d_up = (dh * silu).astype(BF16)
    inner = row_sums(d_gate.astype(F32) * gate + d_up.astype(F32) * up, parts * width)
    mixed = dot(hidden, down_ref[...], NN).astype(BF16).T
    for m in range(parts):
        at = slice(m * width, (m + 1) * width)
        out_ref[m, :width, :] = mixed[at]
        out_ref[m, width:both, :] = (
            dot(gate_up_ref[0, at, :], d_gate, NT) + dot(gate_up_ref[1, at, :], d_up, NT)
        ).astype(BF16)
        out_ref[m, both:, :] = inner


def live_columns(facts_ref, shape):
    column = lax.broadcasted_iota(jnp.int32, shape, 1)
    return column < jnp.where(column < BLOCK, facts_ref[0], facts_ref[1] + BLOCK)


def middle_kernel(
    facts_ref, parts_ref, kept_ref, inverse_ref, second_ref, first_cot_ref, send_ref
):
    parts, rows, count = parts_ref.shape
    width = (rows - PAD) // 2
    total = parts_ref[0].astype(F32)
    for m in range(1, parts):
        total += parts_ref[m].astype(F32)
    inverse = inverse_ref[...]
    first = kept_ref[:width, :].astype(F32)
    second = kept_ref[2 * width : 3 * width, :].astype(F32)
    cot = kept_ref[3 * width :, :].astype(F32)
    second = (second - total[:width]).astype(BF16)
    d_norm = total[width : 2 * width]
    inner = total[2 * width : 2 * width + 1]
    cot = (cot + (d_norm - first * inverse * inner) * inverse).astype(BF16)
    second_ref[...] = second
    first_cot_ref[...] = cot
    masked = jnp.where(live_columns(facts_ref, cot.shape), cot.astype(F32), 0.0).astype(BF16)
    send_ref[:width, :] = second
    send_ref[width:, :] = masked


def last_kernel(
    facts_ref, *refs
):
    *parts, kept_ref, second_ref, first_cot_ref, inverse_ref = refs[:-4]
    first_ref, cot_ref, second_out_ref, first_cot_out_ref = refs[-4:]
    second_out_ref[...] = second_ref[...]
    first_cot_out_ref[...] = first_cot_ref[...]
    width = second_ref.shape[0]
    total = parts[0][...].astype(F32)
    for part in parts[1:]:
        total += part[...].astype(F32)
    attn = total[:width]
    d_norm = total[width : 2 * width]
    inner = total[2 * width : 2 * width + 1]
    inverse = inverse_ref[...]
    first = kept_ref[:width, :].astype(F32)
    cot = kept_ref[width : 2 * width, :].astype(F32)
    live = live_columns(facts_ref, attn.shape)
    first_ref[...] = (first - jnp.where(live, attn, 0.0)).astype(BF16)
    normed = second_ref[...].astype(F32) * inverse
    cot_ref[...] = (cot + (d_norm - normed * inner) * inverse).astype(BF16)


def attention_kernel(groups, facts_ref, rows_ref, query_ref, proj_ref, *refs):
    parts, both, count = rows_ref.shape
    width = both // 2
    pieces, refs = refs[:parts], refs[parts:]
    kept_ref, given_ref, makings_ref, keyval_ref, inner_ref, inverse_ref = refs[:6]
    second_ref, cot_ref, grads_ref = refs[6:]
    me = facts_ref[3]
    for k in range(parts):
        keyval_ref[(me + parts - k) % parts] = pieces[k][...]
    assemble(rows_ref, second_ref, 0)
    assemble(rows_ref, cot_ref, width)
    normed, inverse_ref[...] = normalized(second_ref)
    turned = normed.T
    whole = keyval_ref[...].reshape(parts * width, -1)
    query = dot(turned, query_ref[...].reshape(parts * width, -1), NN).astype(BF16)
    keyval = dot(turned, whole, NN).astype(BF16)
    d_out = dot(cot_ref[...].T, proj_ref[...], NT).astype(BF16)
    half = keyval.shape[1] // 2
    low = lax.broadcasted_iota(jnp.int32, keyval.shape, 1) < half
    wide = keyval.astype(F32)
    rolled = pltpu.roll(wide, half, 1)
    keys = jnp.where(low, wide, rolled).astype(BF16)
    values = jnp.where(low, rolled, wide).astype(BF16)
    row = lax.broadcasted_iota(jnp.int32, (count, count), 0)
    col = lax.broadcasted_iota(jnp.int32, (count, count), 1)
    together = (facts_ref[2] == 1) | ((row >= BLOCK) == (col >= BLOCK))
    allowed = (col <= row) & together & (live_columns(facts_ref, (count, count)) | (col == row))
    scale = 1.0 / (half**0.5)
    heads = d_query = d_key = d_value = 0.0
    for h in range(2):
        own = low if h == 0 else jnp.logical_not(low)
        zero = jnp.zeros_like(query)
        scores = dot(jnp.where(own, query, zero), keys, NT) * scale
        scores = jnp.where(allowed, scores, -1e30)
        expo = jnp.exp(scores - jnp.max(scores, axis=-1, keepdims=True))
        probs = expo / jnp.sum(expo, axis=-1, keepdims=True)
        probs_b = probs.astype(BF16)
        heads += jnp.where(own, dot(probs_b, values, NN), 0.0)
        d_prob = dot(jnp.where(own, d_out, zero), values, NT)
        delta = jnp.sum(probs * d_prob, axis=-1, keepdims=True)
        d_score = (probs * (d_prob - delta) * scale).astype(BF16)
        d_query += jnp.where(own, dot(d_score, keys, NN), 0.0)
        d_key += jnp.where(own, dot(d_score, query, TN), 0.0)
        d_value += jnp.where(own, dot(probs_b, d_out, TN), 0.0)
    heads = heads.astype(BF16)
    d_query = d_query.astype(BF16)
    d_key = d_key + pltpu.roll(d_key, half, 1)
    d_value = d_value + pltpu.roll(d_value, half, 1)
    d_keyval = jnp.where(low, d_key, d_value).astype(BF16)
    makings_ref[0] = heads
    makings_ref[1] = d_query
    makings_ref[2] = d_keyval
    inner_ref[...] = row_sums(
        d_query.astype(F32) * query.astype(F32) + d_keyval.astype(F32) * wide, parts * width
    )
    lines = 8 * width // 7
    spread = lax.broadcasted_iota(jnp.int32, (lines, width), 0)
    core = (spread >= lines // 2).astype(jnp.int32)
    place = (spread - core * (lines // 2)) // 8
    group = (2 * (place // groups) + core) * groups + place % groups
    source = jnp.where(spread % 8 < 7, 7 * group + spread % 8, -1)
    pick = (lax.broadcasted_iota(jnp.int32, source.shape, 1) == source).astype(BF16)
    for m in range(parts):
        at = slice(m * width, (m + 1) * width)
        grads = [dot(normed[at], d_query, NN), dot(normed[at], d_keyval, NN)]
        grads.append(dot(cot_ref[at, :], heads, NN))
        grads = jnp.concatenate(grads, axis=1).astype(BF16)
        grads = dot(pick, grads, NN).astype(BF16)
        to = slice(m * (lines // 2), (m + 1) * (lines // 2))
        for c in range(2):
            grads_ref[c, to, :] = grads[c * (lines // 2) : (c + 1) * (lines // 2)]
    kept_ref[...] = grads_ref[facts_ref[4]]
    given_ref[...] = grads_ref[1 - facts_ref[4]]


def pieces_kernel(
    facts_ref, makings_ref, keyval_ref, inner_ref, query_ref, proj_ref, *refs
):
    parts, width, _ = query_ref.shape
    both = 2 * width
    out_refs, turned_ref = refs[:parts], refs[parts]
    me = facts_ref[3]
    heads, d_query, d_keyval = makings_ref[0], makings_ref[1], makings_ref[2]
    turned_ref[...] = proj_ref[...].T.reshape(turned_ref.shape)
    for k in range(parts):
        m = (me + k) % parts
        out_refs[k][:width, :] = dot(turned_ref[m], heads, NT).astype(BF16)
        out_refs[k][width:both, :] = (
            dot(query_ref[m], d_query, NT) + dot(keyval_ref[m], d_keyval, NT)
        ).astype(BF16)
        out_refs[k][both:, :] = inner_ref[...]


def add_kernel(left_ref, right_ref, out_ref):
    out_ref[...] = (left_ref[...].astype(F32) + right_ref[...].astype(F32)).astype(BF16)


def finish_kernel(grads_ref, query_ref, out_ref, own_ref):
    total = jnp.sum(grads_ref[...].astype(F32), axis=0)
    total = total.reshape(-1, 8, total.shape[1])[:, :7].reshape(-1, total.shape[1])
    query_ref[...] = total[:, :128]
    out_ref[...] = total[:, 256:]
    for m in range(MP):
        own_ref[m] = total[:, 128:256]


def pair_kernel(shares_ref, out_ref):
    groups = out_ref.shape[1]
    per = MP // groups
    for g in range(groups):
        out_ref[:, g, :] = shares_ref[g * per] + shares_ref[g * per + 1]


def shards(
    y_first,
    y_second,
    grad_first,
    grad_second,
    doc_blocks,
    last_fill,
    plan,
    q_weight,
    kv_weight,
    out_weight,
    gate_up,
    down_weight,
):
    count, width = y_first.shape
    seq_size = lax.axis_size(SEQ)
    groups = kv_weight.shape[0]
    streams = (y_first.T, grad_second.T, y_second.T, grad_first.T)
    facts, pieces, send, kept = to_slots(streams, kv_weight, doc_blocks, last_fill, plan)
    send, facts, pieces = lax.optimization_barrier((send, facts, pieces))
    stream = jax.ShapeDtypeStruct((width, count), BF16)
    line = jax.ShapeDtypeStruct((1, count), F32)
    part = jax.ShapeDtypeStruct((2 * width + PAD, count), BF16)
    with jax.named_scope("gather_one"):
        rows = lax.all_gather(send, "mp", axis=0)
    whole = pltpu.VMEM((MP * width, count), BF16)
    parts, r_one = call(
        feed_forward_kernel,
        (jax.ShapeDtypeStruct((MP, *part.shape), BF16), line),
        rows,
        gate_up,
        down_weight,
        scratch=[whole, whole],
        name="feed_forward",
    )
    with jax.named_scope("sum_one"):
        parts = exchange(parts, "mp")
    second_in, first_cot, send = call(
        middle_kernel,
        (stream, stream, jax.ShapeDtypeStruct((2 * width, count), BF16)),
        facts,
        parts,
        kept,
        r_one,
        smem=1,
        name="middle",
    )
    with jax.named_scope("gather_two"):
        rows = lax.all_gather(send, "mp", axis=0)
    query = q_weight.reshape(MP, width, -1)
    half = jax.ShapeDtypeStruct((4 * BLOCK, 384), BF16)
    kept_grads, given, makings, keyval, inner, r_two = call(
        partial(attention_kernel, BLOCK // seq_size),
        (
            half,
            half,
            jax.ShapeDtypeStruct((3, count, 128), BF16),
            jax.ShapeDtypeStruct((MP, width, 128), BF16),
            jax.ShapeDtypeStruct((PAD, count), BF16),
            line,
        ),
        facts,
        rows,
        query,
        out_weight,
        *pieces,
        scratch=[whole, whole, pltpu.VMEM((2, *half.shape), BF16)],
        smem=1,
        name="attention",
    )
    with jax.named_scope("core_sum"):
        given = lax.ppermute(given, "seq_2", [(0, 1), (1, 0)])
    grads = call(add_kernel, half, kept_grads, given, name="add")
    with jax.named_scope("weight_grads"):
        grads = exchange(grads.reshape(seq_size // 2, -1, grads.shape[1]), SEQ[:2])
    parts = call(
        pieces_kernel,
        (part,) * MP,
        facts,
        makings,
        keyval,
        inner,
        query,
        out_weight,
        scratch=[pltpu.VMEM((MP, width, 128), BF16)],
        smem=1,
        name="pieces",
    )
    with jax.named_scope("last_sum"):
        parts = [parts[0]] + [turn(parts[k], k) for k in range(1, MP)]
    first_in, second_cot, second_in, first_cot = call(
        last_kernel,
        (stream,) * 4,
        facts,
        *parts,
        kept,
        second_in,
        first_cot,
        r_two,
        smem=1,
        name="last",
    )
    share = jax.ShapeDtypeStruct((7 * BLOCK // seq_size, 128), F32)
    query_grad, out_grad, own = call(
        finish_kernel,
        (share, share, jax.ShapeDtypeStruct((MP, *share.shape), F32)),
        grads,
        name="finish",
    )
    with jax.named_scope("key_grads"):
        shares = exchange(own, "mp")
    kv_grad = call(
        pair_kernel,
        jax.ShapeDtypeStruct((shares.shape[1], groups, 128), F32),
        shares,
        name="pair",
    )
    return (
        first_in.T,
        second_in.T,
        first_cot.T,
        second_cot.T,
        query_grad,
        kv_grad.transpose(1, 0, 2),
        out_grad.T,
    )


def solution(mesh):
    if "seq" in mesh.shape and mesh.shape["seq"] == 128:
        shape = (8, 8, 2, MP)
    else:
        shape = (2, 2, 2, MP)
    finer = Mesh(mesh.devices.reshape(shape), ("seq_0", "seq_1", "seq_2", "mp"))
    return jax.shard_map(
        shards,
        mesh=finer,
        in_specs=(
            P(SEQ, "mp"),
            P(SEQ, "mp"),
            P(SEQ, "mp"),
            P(SEQ, "mp"),
            P(),
            P(),
            P(),
            P(None, "mp"),
            P(None, "mp", None),
            P("mp", None),
            P(None, None, "mp"),
            P("mp", None),
        ),
        out_specs=(
            P(SEQ, "mp"),
            P(SEQ, "mp"),
            P(SEQ, "mp"),
            P(SEQ, "mp"),
            P(SEQ, "mp"),
            P(None, SEQ, None),
            P("mp", SEQ),
        ),
        check_vma=False,
    )
```
